8 devices in a mesh: batch: 1 (over z), row: 2 (over y), col: 4 (over x, core).
Axes of the slice: x: 2, y: 2, z: 1, core: 2. Of those that a mesh axis runs over, the one named last changes fastest.
Arguments:
- a_mat: bfloat16 [5120, 32768], P(('batch', 'row'), 'col')
Outputs:
- output: bfloat16 [5120, 5120], P(('batch', 'row'), 'col')
All inputs are finite; a program needn't handle non-finite values.
Results may differ from the reference program's by a relative error of at most 0.001.
Values are sent between devices in bfloat16 or wider.
A program may use at most 1 GiB of HBM per device.

```python
import jax
import jax.numpy as jnp
from jax import lax

N = 5120
BLOCK = 256
M_COLS = 32768
ROW_GROUPS = 2
COL_GROUPS = 4


def setup_inputs(seed: int = 0, part: int = 0) -> dict:
    base_key = jax.random.fold_in(jax.random.key(seed), part)
    values = jax.random.normal(base_key, (N, M_COLS), jnp.float32) * (M_COLS ** -0.25)
    return {"a_mat": values.astype(jnp.bfloat16)}


def global_index(size, groups):
    stored = jnp.arange(size)
    per_group = size // groups
    group_id = stored // per_group
    within = stored % per_group
    return ((within // BLOCK) * groups + group_id) * BLOCK + within % BLOCK


def reference(a_mat):
    blocks = N // BLOCK
    natural = a_mat.reshape(ROW_GROUPS, blocks // ROW_GROUPS, BLOCK, M_COLS).transpose(1, 0, 2, 3)
    col_order = natural.reshape(blocks // COL_GROUPS, COL_GROUPS, BLOCK, M_COLS).transpose(1, 0, 2, 3).reshape(N, M_COLS)
    col_trans = col_order.T
    row_index = global_index(N, ROW_GROUPS).reshape(blocks, BLOCK)
    col_index = global_index(N, COL_GROUPS)

    def one_block(block_item):
        row_blk, idx_blk = block_item
        product = jnp.dot(row_blk, col_trans, preferred_element_type=jnp.float32)
        return jnp.where(idx_blk[:, None] >= col_index[None, :], product, 0.0).astype(jnp.bfloat16)

    result = lax.map(one_block, (a_mat.reshape(blocks, BLOCK, M_COLS), row_index))
    return result.reshape(N, N)
```

```python
import functools

import jax
import jax.numpy as jnp
from jax import lax
from jax.experimental import pallas as pl
from jax.experimental.pallas import tpu as pltpu
from jax.sharding import PartitionSpec as P

BLOCK = 256
RING = 3
MESH = pl.DeviceIdType.MESH
DIMS = (((1,), (1,)), ((), ()))


def dot_t(lhs, rhs):
    return lax.dot_general(lhs, rhs, DIMS, preferred_element_type=jnp.float32)


def loop(lower, upper, body):
    def step(i, carry):
        body(i)
        return carry

    lax.fori_loop(lower, upper, step, 0)


def kernel(a, out, got_a, got_core, got_x, got_y, kept, ready, own, part, other, cols, rows,
           load_sem, send_a, recv_a, send_core, recv_core, send_x, recv_x, send_y, recv_y):
    nb = a.shape[0]
    cb = nb // 2
    half = a.shape[2] // 2
    y = lax.axis_index("row")
    c = lax.axis_index("col")
    x = lax.div(c, 2)
    k = lax.rem(c, 2)
    same = k == y
    core_dev = {"col": 2 * x + 1 - k}
    x_dev = {"col": 2 * (1 - x) + k}
    y_dev = {"row": 1 - y}

    barrier = pltpu.get_barrier_semaphore()
    for dev in (core_dev, x_dev, y_dev):
        pl.semaphore_signal(barrier, inc=1, device_id=dev, device_id_type=MESH)
    pl.semaphore_wait(barrier, 3)

    def remote(src, dst, send, recv, dev):
        return pltpu.make_async_remote_copy(src_ref=src, dst_ref=dst, send_sem=send, recv_sem=recv,
                                            device_id=dev, device_id_type=MESH)

    def fetch(src, dst, sem=0):
        copy = pltpu.make_async_copy(src, dst, load_sem.at[sem])
        copy.start()
        return copy

    def a_copy(b):
        return remote(a.at[b, :, pl.ds(pl.multiple_of((1 - y) * half, half), half)], got_a.at[b],
                      send_a.at[b], recv_a.at[b], y_dev)

    loop(0, nb, lambda b: a_copy(b).start())
    first = fetch(a.at[:, :, pl.ds(pl.multiple_of(y * half, half), half)], own.at[pl.ds(0, nb)], 0)
    second = fetch(a.at[:, :, pl.ds(pl.multiple_of((1 - y) * half, half), half)], own.at[pl.ds(nb, nb)], 1)

    def core_copy(job):
        slot = lax.rem(job, RING)
        return remote(part.at[slot], got_core.at[job], send_core.at[slot], recv_core.at[job], core_dev)

    def x_copy(job, i):
        slot = lax.rem(job, RING)
        return remote(part.at[slot, i], got_x.at[job, i], send_x.at[slot, i], recv_x.at[job, i], x_dev)

    def y_copy(b, i):
        s = lax.div(i, 2)
        return remote(ready.at[b, i], got_y.at[b, s], send_y.at[b, s], recv_y.at[b, s], y_dev)

    def add_other(slot, lower, upper):
        def one(i):
            part[slot, i] = part[slot, i] + other[i]

        loop(lower, upper, one)

    def same_send(lo):
        return jnp.logical_and(same, lax.rem(lo, 2) != x)

    def same_recv(lo):
        return jnp.logical_and(same, lax.rem(lo, 2) == x)

    def same_drain(lo):
        @pl.when(jnp.logical_not(same))
        def _():
            core_copy(lo).wait_send()

        @pl.when(same_send(lo))
        def _():
            loop(lo, nb, lambda i: x_copy(lo, i).wait_send())

    def same_compute(lo):
        slot = lax.rem(lo, RING)

        @pl.when(lo >= RING)
        def _():
            same_drain(lo - RING)

        def one(i):
            part[slot, i] = dot_t(own[i], own[lo]) + dot_t(own[nb + i], own[nb + lo])

        loop(lo, nb, one)

        @pl.when(jnp.logical_not(same))
        def _():
            core_copy(lo).start()

    def same_reduce(lo):
        slot = lax.rem(lo, RING)

        @pl.when(same)
        def _():
            core_copy(lo).wait_recv()
            fetch(got_core.at[lo], other).wait()
            add_other(slot, lo, nb)

        @pl.when(same_send(lo))
        def _():
            loop(lo, nb, lambda i: x_copy(lo, i).start())

    def same_final(lo):
        slot = lax.rem(lo, RING)

        @pl.when(same_recv(lo))
        def _():
            loop(lo, nb, lambda i: x_copy(lo, i).wait_recv())
            fetch(got_x.at[lo], other).wait()
            above = (lax.broadcasted_iota(jnp.int32, (BLOCK, BLOCK), 0)
                     < lax.broadcasted_iota(jnp.int32, (BLOCK, BLOCK), 1))

            def one(i):
                drop = jnp.logical_or(i < lo, jnp.logical_and(i == lo, above))
                cols[pl.ds(pl.multiple_of(i * BLOCK, BLOCK), BLOCK), :] = jnp.where(
                    drop, 0.0, part[slot, i] + other[i]).astype(cols.dtype)

            loop(0, nb, one)
            s = lax.div(lo, 2)
            fetch(cols, out.at[:, pl.ds(pl.multiple_of(s * BLOCK, BLOCK), BLOCK)]).wait()

    first.wait()
    second.wait()

    def same_step(t):
        @pl.when(t < nb)
        def _():
            same_compute(t)

        @pl.when(jnp.logical_and(t >= 1, t <= nb))
        def _():
            same_reduce(t - 1)

        @pl.when(t >= 2)
        def _():
            same_final(t - 2)

    loop(0, nb + 2, same_step)

    def mixed_send(b, i):
        split = b + 1 - y
        stay = jnp.logical_and(jnp.logical_not(same), jnp.logical_and(i >= split, lax.rem(b, 2) != x))
        cross = jnp.logical_and(same, jnp.logical_and(i < split, lax.rem(i, 2) != x))
        return jnp.logical_or(stay, cross)

    def mixed_recv(b, i):
        split = b + 1 - y
        stay = jnp.logical_and(jnp.logical_not(same), jnp.logical_and(i >= split, lax.rem(b, 2) == x))
        cross = jnp.logical_and(same, jnp.logical_and(i < split, lax.rem(i, 2) == x))
        return jnp.logical_or(stay, cross)

    def each(cond, action):
        def one(i):
            @pl.when(cond(i))
            def _():
                action(i)

        loop(0, nb, one)

    def mixed_drain(b):
        each(lambda i: mixed_send(b, i), lambda i: x_copy(nb + b, i).wait_send())

    def mixed_step(b):
        job = nb + b
        slot = lax.rem(job, RING)
        split = b + 1 - y

        @pl.when(b < RING)
        def _():
            same_drain(job - RING)

        @pl.when(b >= RING)
        def _():
            mixed_drain(b - RING)

        a_copy(b).wait_recv()
        fetch(got_a.at[b], own.at[2 * nb]).wait()

        def one(i):
            lhs = jnp.where(i >= split, i, 2 * nb)
            rhs = jnp.where(i >= split, 2 * nb, i)
            part[slot, i] = dot_t(own[lhs], own[rhs])

        loop(0, nb, one)
        swap = core_copy(job)
        swap.start()
        swap.wait_recv()
        load = fetch(got_core.at[job], other)
        swap.wait_send()
        load.wait()
        add_other(slot, 0, nb)

        each(lambda i: mixed_send(b, i), lambda i: x_copy(job, i).start())
        each(lambda i: mixed_recv(b, i), lambda i: x_copy(job, i).wait_recv())
        fetch(got_x.at[job], other).wait()

        @pl.when(jnp.logical_and(jnp.logical_not(same), lax.rem(b, 2) == x))
        def _():
            add_other(slot, split, nb)
            fetch(part.at[slot], kept.at[:, lax.div(b, 2)]).wait()

        @pl.when(same)
        def _():
            def add(i):
                part[slot, i] = part[slot, i] + other[i]

            each(lambda i: mixed_recv(b, i), add)
            fetch(part.at[slot], ready.at[b]).wait()
            each(lambda i: mixed_recv(b, i), lambda i: y_copy(b, i).start())

    loop(0, nb, mixed_step)

    @pl.when(jnp.logical_not(same))
    def _():
        def final(hi):
            def wait_one(s):
                i = 2 * s + x

                @pl.when(i < hi + y)
                def _():
                    remote(ready.at[hi, i], got_y.at[hi, s], send_y.at[hi, s], recv_y.at[hi, s], y_dev).wait_recv()

            loop(0, cb, wait_one)
            mine = fetch(kept.at[hi], other.at[pl.ds(0, cb)], 0)
            theirs = fetch(got_y.at[hi], other.at[pl.ds(cb, cb)], 1)
            mine.wait()
            theirs.wait()
            for s in range(cb):
                rows[:, s * BLOCK:(s + 1) * BLOCK] = jnp.where(
                    2 * s + x < hi + y, other[s] + other[cb + s], 0.0).astype(rows.dtype)
            fetch(rows, out.at[pl.ds(pl.multiple_of(hi * BLOCK, BLOCK), BLOCK), :]).wait()

        loop(0, nb, final)

    def finish(b):
        @pl.when(b >= nb - RING)
        def _():
            mixed_drain(b)

        @pl.when(same)
        def _():
            each(lambda i: mixed_recv(b, i), lambda i: y_copy(b, i).wait_send())

        a_copy(b).wait_send()

    loop(0, nb, finish)


def solution(mesh):
    def local_fn(a_local):
        local_rows, m_local = a_local.shape
        nb = local_rows // BLOCK
        cb = nb // 2
        half = m_local // 2
        f32, bf16 = jnp.float32, a_local.dtype
        hbm = pl.BlockSpec(memory_space=pl.ANY)
        shapes = [
            jax.ShapeDtypeStruct((local_rows, cb * BLOCK), bf16),
            jax.ShapeDtypeStruct((nb, BLOCK, half), bf16),
            jax.ShapeDtypeStruct((2 * nb, nb, BLOCK, BLOCK), f32),
            jax.ShapeDtypeStruct((2 * nb, nb, BLOCK, BLOCK), f32),
            jax.ShapeDtypeStruct((nb, cb, BLOCK, BLOCK), f32),
            jax.ShapeDtypeStruct((nb, cb, BLOCK, BLOCK), f32),
            jax.ShapeDtypeStruct((nb, nb, BLOCK, BLOCK), f32),
        ]
        dma = pltpu.SemaphoreType.DMA
        outs = pl.pallas_call(
            kernel,
            out_shape=shapes,
            in_specs=[hbm],
            out_specs=[hbm] * len(shapes),
            scratch_shapes=[
                pltpu.VMEM((2 * nb + 1, BLOCK, half), bf16),
                pltpu.VMEM((RING, nb, BLOCK, BLOCK), f32),
                pltpu.VMEM((nb, BLOCK, BLOCK), f32),
                pltpu.VMEM((local_rows, BLOCK), bf16),
                pltpu.VMEM((BLOCK, cb * BLOCK), bf16),
                dma((2,)),
                dma((nb,)), dma((nb,)),
                dma((RING,)), dma((2 * nb,)),
                dma((RING, nb)), dma((2 * nb, nb)),
                dma((nb, cb)), dma((nb, cb)),
            ],
            compiler_params=pltpu.CompilerParams(collective_id=0, has_side_effects=True,
                                                 vmem_limit_bytes=67043328),
            cost_estimate=pl.CostEstimate(flops=210 * 2 * BLOCK * BLOCK * half, bytes_accessed=400 * 2**20,
                                          transcendentals=0),
        )(a_local.reshape(nb, BLOCK, m_local))
        return outs[0]

    part_spec = P(("batch", "row"), "col")
    return jax.shard_map(local_fn, mesh=mesh, in_specs=(part_spec,), out_specs=part_spec, check_vma=False)
```

```python
import functools

import jax
import jax.numpy as jnp
from jax import lax
from jax.experimental import pallas as pl
from jax.experimental.pallas import tpu as pltpu
from jax.sharding import PartitionSpec as P

BLOCK = 256
RING = 3
MESH = pl.DeviceIdType.MESH
DIMS = (((1,), (1,)), ((), ()))


def dot_t(lhs, rhs):
    return lax.dot_general(lhs, rhs, DIMS, preferred_element_type=jnp.float32)


def loop(lower, upper, body):
    def step(i, carry):
        body(i)
        return carry

    lax.fori_loop(lower, upper, step, 0)


def kernel(a, out, got_a, got_core, got_x, got_y, kept, ready, own, part, other, cols, rows,
           load_sem, send_a, recv_a, send_core, recv_core, send_x, recv_x, send_y, recv_y):
    nb = a.shape[0]
    cb = nb // 2
    half = a.shape[2] // 2
    y = lax.axis_index("row")
    c = lax.axis_index("col")
    x = lax.div(c, 2)
    k = lax.rem(c, 2)
    same = k == y
    core_dev = {"col": 2 * x + 1 - k}
    x_dev = {"col": 2 * (1 - x) + k}
    y_dev = {"row": 1 - y}

    barrier = pltpu.get_barrier_semaphore()
    for dev in (core_dev, x_dev, y_dev):
        pl.semaphore_signal(barrier, inc=1, device_id=dev, device_id_type=MESH)
    pl.semaphore_wait(barrier, 3)

    def remote(src, dst, send, recv, dev):
        return pltpu.make_async_remote_copy(src_ref=src, dst_ref=dst, send_sem=send, recv_sem=recv,
                                            device_id=dev, device_id_type=MESH)

    def fetch(src, dst, sem=0):
        copy = pltpu.make_async_copy(src, dst, load_sem.at[sem])
        copy.start()
        return copy

    def a_copy(b):
        return remote(a.at[b, :, pl.ds(pl.multiple_of((1 - y) * half, half), half)], got_a.at[b],
                      send_a.at[b], recv_a.at[b], y_dev)

    loop(0, nb, lambda b: a_copy(b).start())
    first = fetch(a.at[:, :, pl.ds(pl.multiple_of(y * half, half), half)], own.at[pl.ds(0, nb)], 0)
    second = fetch(a.at[:, :, pl.ds(pl.multiple_of((1 - y) * half, half), half)], own.at[pl.ds(nb, nb)], 1)

    def core_copy(job):
        slot = lax.rem(job, RING)
        return remote(part.at[slot], got_core.at[job], send_core.at[slot], recv_core.at[job], core_dev)

    def x_copy(job, i):
        slot = lax.rem(job, RING)
        return remote(part.at[slot, i], got_x.at[job, i], send_x.at[slot, i], recv_x.at[job, i], x_dev)

    def y_copy(b, i):
        s = lax.div(i, 2)
        return remote(ready.at[b, i], got_y.at[b, s], send_y.at[b, s], recv_y.at[b, s], y_dev)

    def add_other(slot, lower, upper):
        def one(i):
            part[slot, i] = part[slot, i] + other[i]

        loop(lower, upper, one)

    def same_send(lo):
        return jnp.logical_and(same, lax.rem(lo, 2) != x)

    def same_recv(lo):
        return jnp.logical_and(same, lax.rem(lo, 2) == x)

    def same_drain(lo):
        @pl.when(jnp.logical_not(same))
        def _():
            core_copy(lo).wait_send()

        @pl.when(same_send(lo))
        def _():
            loop(lo, nb, lambda i: x_copy(lo, i).wait_send())

    def same_compute(lo):
        slot = lax.rem(lo, RING)

        @pl.when(lo >= RING)
        def _():
            same_drain(lo - RING)

        def one(i):
            part[slot, i] = dot_t(own[i], own[lo]) + dot_t(own[nb + i], own[nb + lo])

        loop(lo, nb, one)

        @pl.when(jnp.logical_not(same))
        def _():
            core_copy(lo).start()

    def same_reduce(lo):
        slot = lax.rem(lo, RING)

        @pl.when(same)
        def _():
            core_copy(lo).wait_recv()
            fetch(got_core.at[lo], other).wait()
            add_other(slot, lo, nb)

        @pl.when(same_send(lo))
        def _():
            loop(lo, nb, lambda i: x_copy(lo, i).start())

    def same_final(lo):
        slot = lax.rem(lo, RING)

        @pl.when(same_recv(lo))
        def _():
            loop(lo, nb, lambda i: x_copy(lo, i).wait_recv())
            fetch(got_x.at[lo], other).wait()
            above = (lax.broadcasted_iota(jnp.int32, (BLOCK, BLOCK), 0)
                     < lax.broadcasted_iota(jnp.int32, (BLOCK, BLOCK), 1))

            def one(i):
                drop = jnp.logical_or(i < lo, jnp.logical_and(i == lo, above))
                cols[pl.ds(pl.multiple_of(i * BLOCK, BLOCK), BLOCK), :] = jnp.where(
                    drop, 0.0, part[slot, i] + other[i]).astype(cols.dtype)

            loop(0, nb, one)
            s = lax.div(lo, 2)
            fetch(cols, out.at[:, pl.ds(pl.multiple_of(s * BLOCK, BLOCK), BLOCK)]).wait()

    first.wait()
    second.wait()

    def same_step(t):
        @pl.when(t < nb)
        def _():
            same_compute(t)

        @pl.when(jnp.logical_and(t >= 1, t <= nb))
        def _():
            same_reduce(t - 1)

        @pl.when(t >= 2)
        def _():
            same_final(t - 2)

    loop(0, nb + 2, same_step)

    def mixed_send(b, i):
        split = b + 1 - y
        stay = jnp.logical_and(jnp.logical_not(same), jnp.logical_and(i >= split, lax.rem(b, 2) != x))
        cross = jnp.logical_and(same, jnp.logical_and(i < split, lax.rem(i, 2) != x))
        return jnp.logical_or(stay, cross)

    def mixed_recv(b, i):
        split = b + 1 - y
        stay = jnp.logical_and(jnp.logical_not(same), jnp.logical_and(i >= split, lax.rem(b, 2) == x))
        cross = jnp.logical_and(same, jnp.logical_and(i < split, lax.rem(i, 2) == x))
        return jnp.logical_or(stay, cross)

    def each(cond, action):
        def one(i):
            @pl.when(cond(i))
            def _():
                action(i)

        loop(0, nb, one)

    def mixed_drain(b):
        each(lambda i: mixed_send(b, i), lambda i: x_copy(nb + b, i).wait_send())

    def mixed_reduce(b):
        job = nb + b
        slot = lax.rem(job, RING)
        split = b + 1 - y
        each(lambda i: mixed_recv(b, i), lambda i: x_copy(job, i).wait_recv())
        fetch(got_x.at[job], other).wait()

        @pl.when(jnp.logical_and(jnp.logical_not(same), lax.rem(b, 2) == x))
        def _():
            add_other(slot, split, nb)
            fetch(part.at[slot], kept.at[:, lax.div(b, 2)]).wait()

        @pl.when(same)
        def _():
            def add(i):
                part[slot, i] = part[slot, i] + other[i]

            each(lambda i: mixed_recv(b, i), add)
            fetch(part.at[slot], ready.at[b]).wait()
            each(lambda i: mixed_recv(b, i), lambda i: y_copy(b, i).start())

    def mixed_step(b):
        job = nb + b
        slot = lax.rem(job, RING)
        split = b + 1 - y

        @pl.when(b < RING)
        def _():
            same_drain(job - RING)

        @pl.when(b >= RING)
        def _():
            mixed_drain(b - RING)

        a_copy(b).wait_recv()
        fetch(got_a.at[b], own.at[2 * nb]).wait()

        def one(i):
            lhs = jnp.where(i >= split, i, 2 * nb)
            rhs = jnp.where(i >= split, 2 * nb, i)
            part[slot, i] = dot_t(own[lhs], own[rhs])

        loop(0, nb, one)
        core_copy(job).start()

        @pl.when(b >= 1)
        def _():
            mixed_reduce(b - 1)

        swap = core_copy(job)
        swap.wait_recv()
        load = fetch(got_core.at[job], other)
        swap.wait_send()
        load.wait()
        add_other(slot, 0, nb)
        each(lambda i: mixed_send(b, i), lambda i: x_copy(job, i).start())

    loop(0, nb, mixed_step)
    mixed_reduce(jnp.int32(nb - 1))

    @pl.when(jnp.logical_not(same))
    def _():
        def final(hi):
            def wait_one(s):
                i = 2 * s + x

                @pl.when(i < hi + y)
                def _():
                    remote(ready.at[hi, i], got_y.at[hi, s], send_y.at[hi, s], recv_y.at[hi, s], y_dev).wait_recv()

            loop(0, cb, wait_one)
            mine = fetch(kept.at[hi], other.at[pl.ds(0, cb)], 0)
            theirs = fetch(got_y.at[hi], other.at[pl.ds(cb, cb)], 1)
            mine.wait()
            theirs.wait()
            for s in range(cb):
                rows[:, s * BLOCK:(s + 1) * BLOCK] = jnp.where(
                    2 * s + x < hi + y, other[s] + other[cb + s], 0.0).astype(rows.dtype)
            fetch(rows, out.at[pl.ds(pl.multiple_of(hi * BLOCK, BLOCK), BLOCK), :]).wait()

        loop(0, nb, final)

    def finish(b):
        @pl.when(b >= nb - RING)
        def _():
            mixed_drain(b)

        @pl.when(same)
        def _():
            each(lambda i: mixed_recv(b, i), lambda i: y_copy(b, i).wait_send())

        a_copy(b).wait_send()

    loop(0, nb, finish)


def solution(mesh):
    def local_fn(a_local):
        local_rows, m_local = a_local.shape
        nb = local_rows // BLOCK
        cb = nb // 2
        half = m_local // 2
        f32, bf16 = jnp.float32, a_local.dtype
        hbm = pl.BlockSpec(memory_space=pl.ANY)
        shapes = [
            jax.ShapeDtypeStruct((local_rows, cb * BLOCK), bf16),
            jax.ShapeDtypeStruct((nb, BLOCK, half), bf16),
            jax.ShapeDtypeStruct((2 * nb, nb, BLOCK, BLOCK), f32),
            jax.ShapeDtypeStruct((2 * nb, nb, BLOCK, BLOCK), f32),
            jax.ShapeDtypeStruct((nb, cb, BLOCK, BLOCK), f32),
            jax.ShapeDtypeStruct((nb, cb, BLOCK, BLOCK), f32),
            jax.ShapeDtypeStruct((nb, nb, BLOCK, BLOCK), f32),
        ]
        dma = pltpu.SemaphoreType.DMA
        outs = pl.pallas_call(
            kernel,
            out_shape=shapes,
            in_specs=[hbm],
            out_specs=[hbm] * len(shapes),
            scratch_shapes=[
                pltpu.VMEM((2 * nb + 1, BLOCK, half), bf16),
                pltpu.VMEM((RING, nb, BLOCK, BLOCK), f32),
                pltpu.VMEM((nb, BLOCK, BLOCK), f32),
                pltpu.VMEM((local_rows, BLOCK), bf16),
                pltpu.VMEM((BLOCK, cb * BLOCK), bf16),
                dma((2,)),
                dma((nb,)), dma((nb,)),
                dma((RING,)), dma((2 * nb,)),
                dma((RING, nb)), dma((2 * nb, nb)),
                dma((nb, cb)), dma((nb, cb)),
            ],
            compiler_params=pltpu.CompilerParams(collective_id=0, has_side_effects=True,
                                                 vmem_limit_bytes=67043328),
            cost_estimate=pl.CostEstimate(flops=210 * 2 * BLOCK * BLOCK * half, bytes_accessed=400 * 2**20,
                                          transcendentals=0),
        )(a_local.reshape(nb, BLOCK, m_local))
        return outs[0]

    part_spec = P(("batch", "row"), "col")
    return jax.shard_map(local_fn, mesh=mesh, in_specs=(part_spec,), out_specs=part_spec, check_vma=False)
```

```python
import functools

import jax
import jax.numpy as jnp
from jax import lax
from jax.experimental import pallas as pl
from jax.experimental.pallas import tpu as pltpu
from jax.sharding import PartitionSpec as P

BLOCK = 256
RING = 3
LANES = 128
AHEAD = 2
MESH = pl.DeviceIdType.MESH
DIMS = (((1,), (1,)), ((), ()))


def dot_t(lhs, rhs):
    return lax.dot_general(lhs, rhs, DIMS, preferred_element_type=jnp.float32)


def loop(lower, upper, body):
    def step(i, carry):
        body(i)
        return carry

    lax.fori_loop(lower, upper, step, 0)


def kernel(a, out, got_a, got_core, got_x, got_y, kept, ready, moved, relayed, own, part, other, cols, rows, extra,
           load_sem, send_a, recv_a, send_core, recv_core, send_x, recv_x, send_y, recv_y, send_m, recv_m):
    nb = a.shape[0]
    cb = nb // 2
    half = a.shape[2] // 2
    y = lax.axis_index("row")
    c = lax.axis_index("col")
    x = lax.div(c, 2)
    k = lax.rem(c, 2)
    same = k == y
    core_dev = {"col": 2 * x + 1 - k}
    x_dev = {"col": 2 * (1 - x) + k}
    y_dev = {"row": 1 - y}

    barrier = pltpu.get_barrier_semaphore()
    for dev in (core_dev, x_dev, y_dev):
        pl.semaphore_signal(barrier, inc=1, device_id=dev, device_id_type=MESH)
    pl.semaphore_wait(barrier, 3)

    def remote(src, dst, send, recv, dev):
        return pltpu.make_async_remote_copy(src_ref=src, dst_ref=dst, send_sem=send, recv_sem=recv,
                                            device_id=dev, device_id_type=MESH)

    def fetch(src, dst, sem=0):
        copy = pltpu.make_async_copy(src, dst, load_sem.at[sem])
        copy.start()
        return copy

    narrow_send = jnp.logical_and(x == 0, y == 0)
    narrow_recv = jnp.logical_and(x == 0, y == 1)
    takes_moved = jnp.logical_and(x == 1, y == 0)
    relays = jnp.logical_and(x == 1, y == 1)

    def wide_copy(b):
        return remote(a.at[b, :, pl.ds(pl.multiple_of((1 - y) * half, half), half)], got_a.at[b],
                      send_a.at[b], recv_a.at[b], y_dev)

    def narrow_copy(b):
        return remote(a.at[b, :, pl.ds(half + LANES, half - LANES)], got_a.at[b, :, pl.ds(LANES, half - LANES)],
                      send_a.at[b], recv_a.at[b], y_dev)

    def a_copy(b, narrow, action):
        @pl.when(narrow)
        def _():
            action(narrow_copy(b))

        @pl.when(jnp.logical_not(narrow))
        def _():
            action(wide_copy(b))

    def start_a(b):
        a_copy(b, narrow_send, lambda copy: copy.start())

    move = remote(a.at[:, :, pl.ds(half, LANES)], moved, send_m.at[0], recv_m.at[0], x_dev)
    relay = remote(moved, relayed, send_m.at[1], recv_m.at[1], y_dev)

    @pl.when(x == 0)
    def _():
        move.start()

    loop(0, AHEAD, start_a)
    first = fetch(a.at[:, :, pl.ds(pl.multiple_of(y * half, half), half)], own.at[pl.ds(0, nb)], 0)
    second = fetch(a.at[:, :, pl.ds(pl.multiple_of((1 - y) * half, half), half)], own.at[pl.ds(nb, nb)], 1)

    def core_copy(job):
        slot = lax.rem(job, RING)
        return remote(part.at[slot], got_core.at[job], send_core.at[slot], recv_core.at[job], core_dev)

    def x_copy(job, i):
        slot = lax.rem(job, RING)
        return remote(part.at[slot, i], got_x.at[job, i], send_x.at[slot, i], recv_x.at[job, i], x_dev)

    def y_copy(b, i):
        s = lax.div(i, 2)
        return remote(ready.at[b, i], got_y.at[b, s], send_y.at[b, s], recv_y.at[b, s], y_dev)

    def add_other(slot, lower, upper):
        def one(i):
            part[slot, i] = part[slot, i] + other[i]

        loop(lower, upper, one)

    def same_send(lo):
        return jnp.logical_and(same, lax.rem(lo, 2) != x)

    def same_recv(lo):
        return jnp.logical_and(same, lax.rem(lo, 2) == x)

    def same_drain(lo):
        @pl.when(jnp.logical_not(same))
        def _():
            core_copy(lo).wait_send()

        @pl.when(same_send(lo))
        def _():
            loop(lo, nb, lambda i: x_copy(lo, i).wait_send())

    def same_compute(lo):
        slot = lax.rem(lo, RING)

        @pl.when(lo >= RING)
        def _():
            same_drain(lo - RING)

        def one(i):
            part[slot, i] = dot_t(own[i], own[lo]) + dot_t(own[nb + i], own[nb + lo])

        loop(lo, nb, one)

        @pl.when(jnp.logical_not(same))
        def _():
            core_copy(lo).start()

    def same_reduce(lo):
        slot = lax.rem(lo, RING)

        @pl.when(same)
        def _():
            core_copy(lo).wait_recv()
            fetch(got_core.at[lo], other).wait()
            add_other(slot, lo, nb)

        @pl.when(same_send(lo))
        def _():
            loop(lo, nb, lambda i: x_copy(lo, i).start())

    def same_final(lo):
        slot = lax.rem(lo, RING)

        @pl.when(same_recv(lo))
        def _():
            loop(lo, nb, lambda i: x_copy(lo, i).wait_recv())
            fetch(got_x.at[lo], other).wait()
            above = (lax.broadcasted_iota(jnp.int32, (BLOCK, BLOCK), 0)
                     < lax.broadcasted_iota(jnp.int32, (BLOCK, BLOCK), 1))

            def one(i):
                drop = jnp.logical_or(i < lo, jnp.logical_and(i == lo, above))
                cols[pl.ds(pl.multiple_of(i * BLOCK, BLOCK), BLOCK), :] = jnp.where(
                    drop, 0.0, part[slot, i] + other[i]).astype(cols.dtype)

            loop(0, nb, one)
            s = lax.div(lo, 2)
            fetch(cols, out.at[:, pl.ds(pl.multiple_of(s * BLOCK, BLOCK), BLOCK)]).wait()

    first.wait()
    second.wait()

    @pl.when(x == 1)
    def _():
        move.wait_recv()

    @pl.when(relays)
    def _():
        relay.start()

    loop(AHEAD, nb, start_a)

    def same_step(t):
        @pl.when(t < nb)
        def _():
            same_compute(t)

        @pl.when(jnp.logical_and(t >= 1, t <= nb))
        def _():
            same_reduce(t - 1)

        @pl.when(t >= 2)
        def _():
            same_final(t - 2)

    loop(0, nb + 2, same_step)

    def mixed_send(b, i):
        split = b + 1 - y
        stay = jnp.logical_and(jnp.logical_not(same), jnp.logical_and(i >= split, lax.rem(b, 2) != x))
        cross = jnp.logical_and(same, jnp.logical_and(i < split, lax.rem(i, 2) != x))
        return jnp.logical_or(stay, cross)

    def mixed_recv(b, i):
        split = b + 1 - y
        stay = jnp.logical_and(jnp.logical_not(same), jnp.logical_and(i >= split, lax.rem(b, 2) == x))
        cross = jnp.logical_and(same, jnp.logical_and(i < split, lax.rem(i, 2) == x))
        return jnp.logical_or(stay, cross)

    def each(cond, action):
        def one(i):
            @pl.when(cond(i))
            def _():
                action(i)

        loop(0, nb, one)

    def mixed_drain(b):
        each(lambda i: mixed_send(b, i), lambda i: x_copy(nb + b, i).wait_send())

    def mixed_reduce(b):
        job = nb + b
        slot = lax.rem(job, RING)
        split = b + 1 - y
        each(lambda i: mixed_recv(b, i), lambda i: x_copy(job, i).wait_recv())
        fetch(got_x.at[job], other).wait()

        @pl.when(jnp.logical_and(jnp.logical_not(same), lax.rem(b, 2) == x))
        def _():
            add_other(slot, split, nb)
            fetch(part.at[slot], kept.at[:, lax.div(b, 2)]).wait()

        @pl.when(same)
        def _():
            def add(i):
                part[slot, i] = part[slot, i] + other[i]

            each(lambda i: mixed_recv(b, i), add)
            fetch(part.at[slot], ready.at[b]).wait()
            each(lambda i: mixed_recv(b, i), lambda i: y_copy(b, i).start())

    @pl.when(narrow_recv)
    def _():
        own[2 * nb, :, 0:LANES] = jnp.zeros((BLOCK, LANES), own.dtype)

    @pl.when(takes_moved)
    def _():
        relay.wait_recv()
        fetch(moved, extra.at[0]).wait()
        fetch(relayed, extra.at[1]).wait()

    def mixed_step(b):
        job = nb + b
        slot = lax.rem(job, RING)
        split = b + 1 - y

        @pl.when(b < RING)
        def _():
            same_drain(job - RING)

        @pl.when(b >= RING)
        def _():
            mixed_drain(b - RING)

        a_copy(b, narrow_recv, lambda copy: copy.wait_recv())

        @pl.when(narrow_recv)
        def _():
            fetch(got_a.at[b, :, pl.ds(LANES, half - LANES)], own.at[2 * nb, :, pl.ds(LANES, half - LANES)]).wait()

        @pl.when(jnp.logical_not(narrow_recv))
        def _():
            fetch(got_a.at[b], own.at[2 * nb]).wait()

        def one(i):
            lhs = jnp.where(i >= split, i, 2 * nb)
            rhs = jnp.where(i >= split, 2 * nb, i)
            part[slot, i] = dot_t(own[lhs], own[rhs])

        def one_extra(i):
            left = jnp.where(i >= split, 0, 1)
            part[slot, i] = part[slot, i] + dot_t(extra[left, jnp.where(i >= split, i, b)],
                                                  extra[1 - left, jnp.where(i >= split, b, i)])

        loop(0, nb, one)

        @pl.when(takes_moved)
        def _():
            loop(0, nb, one_extra)

        core_copy(job).start()

        @pl.when(b >= 1)
        def _():
            mixed_reduce(b - 1)

        swap = core_copy(job)
        swap.wait_recv()
        load = fetch(got_core.at[job], other)
        swap.wait_send()
        load.wait()
        add_other(slot, 0, nb)
        each(lambda i: mixed_send(b, i), lambda i: x_copy(job, i).start())

    loop(0, nb, mixed_step)
    mixed_reduce(jnp.int32(nb - 1))

    @pl.when(jnp.logical_not(same))
    def _():
        def final(hi):
            def wait_one(s):
                i = 2 * s + x

                @pl.when(i < hi + y)
                def _():
                    remote(ready.at[hi, i], got_y.at[hi, s], send_y.at[hi, s], recv_y.at[hi, s], y_dev).wait_recv()

            loop(0, cb, wait_one)
            mine = fetch(kept.at[hi], other.at[pl.ds(0, cb)], 0)
            theirs = fetch(got_y.at[hi], other.at[pl.ds(cb, cb)], 1)
            mine.wait()
            theirs.wait()
            for s in range(cb):
                rows[:, s * BLOCK:(s + 1) * BLOCK] = jnp.where(
                    2 * s + x < hi + y, other[s] + other[cb + s], 0.0).astype(rows.dtype)
            fetch(rows, out.at[pl.ds(pl.multiple_of(hi * BLOCK, BLOCK), BLOCK), :]).wait()

        loop(0, nb, final)

    def finish(b):
        @pl.when(b >= nb - RING)
        def _():
            mixed_drain(b)

        @pl.when(same)
        def _():
            each(lambda i: mixed_recv(b, i), lambda i: y_copy(b, i).wait_send())

        a_copy(b, narrow_send, lambda copy: copy.wait_send())

    loop(0, nb, finish)

    @pl.when(x == 0)
    def _():
        move.wait_send()

    @pl.when(relays)
    def _():
        relay.wait_send()


def solution(mesh):
    def local_fn(a_local):
        local_rows, m_local = a_local.shape
        nb = local_rows // BLOCK
        cb = nb // 2
        half = m_local // 2
        f32, bf16 = jnp.float32, a_local.dtype
        hbm = pl.BlockSpec(memory_space=pl.ANY)
        shapes = [
            jax.ShapeDtypeStruct((local_rows, cb * BLOCK), bf16),
            jax.ShapeDtypeStruct((nb, BLOCK, half), bf16),
            jax.ShapeDtypeStruct((2 * nb, nb, BLOCK, BLOCK), f32),
            jax.ShapeDtypeStruct((2 * nb, nb, BLOCK, BLOCK), f32),
            jax.ShapeDtypeStruct((nb, cb, BLOCK, BLOCK), f32),
            jax.ShapeDtypeStruct((nb, cb, BLOCK, BLOCK), f32),
            jax.ShapeDtypeStruct((nb, nb, BLOCK, BLOCK), f32),
            jax.ShapeDtypeStruct((nb, BLOCK, LANES), bf16),
            jax.ShapeDtypeStruct((nb, BLOCK, LANES), bf16),
        ]
        dma = pltpu.SemaphoreType.DMA
        outs = pl.pallas_call(
            kernel,
            out_shape=shapes,
            in_specs=[hbm],
            out_specs=[hbm] * len(shapes),
            scratch_shapes=[
                pltpu.VMEM((2 * nb + 1, BLOCK, half), bf16),
                pltpu.VMEM((RING, nb, BLOCK, BLOCK), f32),
                pltpu.VMEM((nb, BLOCK, BLOCK), f32),
                pltpu.VMEM((local_rows, BLOCK), bf16),
                pltpu.VMEM((BLOCK, cb * BLOCK), bf16),
                pltpu.VMEM((2, nb, BLOCK, LANES), bf16),
                dma((2,)),
                dma((nb,)), dma((nb,)),
                dma((RING,)), dma((2 * nb,)),
                dma((RING, nb)), dma((2 * nb, nb)),
                dma((nb, cb)), dma((nb, cb)),
                dma((2,)), dma((2,)),
            ],
            compiler_params=pltpu.CompilerParams(collective_id=0, has_side_effects=True,
                                                 vmem_limit_bytes=67043328),
            cost_estimate=pl.CostEstimate(flops=210 * 2 * BLOCK * BLOCK * half, bytes_accessed=400 * 2**20,
                                          transcendentals=0),
        )(a_local.reshape(nb, BLOCK, m_local))
        return outs[0]

    part_spec = P(("batch", "row"), "col")
    return jax.shard_map(local_fn, mesh=mesh, in_specs=(part_spec,), out_specs=part_spec, check_vma=False)
```

```python
import functools

import jax
import jax.numpy as jnp
from jax import lax
from jax.experimental import pallas as pl
from jax.experimental.pallas import tpu as pltpu
from jax.sharding import PartitionSpec as P

BLOCK = 256
RING = 3
LANES = 128
AHEAD = 2
MESH = pl.DeviceIdType.MESH
DIMS = (((1,), (1,)), ((), ()))


def dot_t(lhs, rhs):
    return lax.dot_general(lhs, rhs, DIMS, preferred_element_type=jnp.float32)


def loop(lower, upper, body):
    def step(i, carry):
        body(i)
        return carry

    lax.fori_loop(lower, upper, step, 0)


def kernel(a, out, got_a, got_core, got_x, got_y, kept, ready, moved, relayed, own, part, other, cols, rows, extra, last_y,
           load_sem, far_sem, send_a, recv_a, send_core, recv_core, send_x, recv_x, send_y, recv_y, send_m, recv_m):
    nb = a.shape[0]
    cb = nb // 2
    half = a.shape[2] // 2
    y = lax.axis_index("row")
    c = lax.axis_index("col")
    x = lax.div(c, 2)
    k = lax.rem(c, 2)
    same = k == y
    core_dev = {"col": 2 * x + 1 - k}
    x_dev = {"col": 2 * (1 - x) + k}
    y_dev = {"row": 1 - y}

    barrier = pltpu.get_barrier_semaphore()
    for dev in (core_dev, x_dev, y_dev):
        pl.semaphore_signal(barrier, inc=1, device_id=dev, device_id_type=MESH)
    pl.semaphore_wait(barrier, 3)

    def remote(src, dst, send, recv, dev):
        return pltpu.make_async_remote_copy(src_ref=src, dst_ref=dst, send_sem=send, recv_sem=recv,
                                            device_id=dev, device_id_type=MESH)

    def fetch(src, dst, sem=0):
        copy = pltpu.make_async_copy(src, dst, load_sem.at[sem])
        copy.start()
        return copy

    narrow_send = jnp.logical_and(x == 0, y == 0)
    narrow_recv = jnp.logical_and(x == 0, y == 1)
    takes_moved = jnp.logical_and(x == 1, y == 0)
    relays = jnp.logical_and(x == 1, y == 1)

    def wide_copy(b):
        return remote(a.at[b, :, pl.ds(pl.multiple_of((1 - y) * half, half), half)], got_a.at[b],
                      send_a.at[b], recv_a.at[b], y_dev)

    def narrow_copy(b):
        return remote(a.at[b, :, pl.ds(half + LANES, half - LANES)], got_a.at[b, :, pl.ds(LANES, half - LANES)],
                      send_a.at[b], recv_a.at[b], y_dev)

    def a_copy(b, narrow, action):
        @pl.when(narrow)
        def _():
            action(narrow_copy(b))

        @pl.when(jnp.logical_not(narrow))
        def _():
            action(wide_copy(b))

    def start_a(b):
        a_copy(b, narrow_send, lambda copy: copy.start())

    move = remote(a.at[:, :, pl.ds(half, LANES)], moved, send_m.at[0], recv_m.at[0], x_dev)
    relay = remote(moved, relayed, send_m.at[1], recv_m.at[1], y_dev)

    @pl.when(x == 0)
    def _():
        move.start()

    loop(0, AHEAD, start_a)
    first = fetch(a.at[:, :, pl.ds(pl.multiple_of(y * half, half), half)], own.at[pl.ds(0, nb)])

    def far_slot(lo, i):
        return nb + 1 + jnp.where(i == lo, lax.rem(lo, 2), 2 + lax.rem(i, 2))

    def far_copy(lo, i):
        slot = far_slot(lo, i)
        return pltpu.make_async_copy(a.at[i, :, pl.ds(pl.multiple_of((1 - y) * half, half), half)], own.at[slot],
                                     far_sem.at[slot - nb - 1])

    far_copy(jnp.int32(0), jnp.int32(0)).start()

    def core_copy(job):
        slot = lax.rem(job, RING)
        return remote(part.at[slot], got_core.at[job], send_core.at[slot], recv_core.at[job], core_dev)

    def x_copy(job, i):
        slot = lax.rem(job, RING)
        return remote(part.at[slot, i], got_x.at[job, i], send_x.at[slot, i], recv_x.at[job, i], x_dev)

    def y_copy(b, i, action):
        s = lax.div(i, 2)

        @pl.when(b < nb - 1)
        def _():
            action(remote(ready.at[b, i], got_y.at[b, s], send_y.at[b, s], recv_y.at[b, s], y_dev))

        @pl.when(b == nb - 1)
        def _():
            action(remote(ready.at[b, i], last_y.at[s], send_y.at[b, s], recv_y.at[b, s], y_dev))

    def add_other(slot, lower, upper):
        def one(i):
            part[slot, i] = part[slot, i] + other[i]

        loop(lower, upper, one)

    def same_send(lo):
        return jnp.logical_and(same, lax.rem(lo, 2) != x)

    def same_recv(lo):
        return jnp.logical_and(same, lax.rem(lo, 2) == x)

    def same_drain(lo):
        @pl.when(jnp.logical_not(same))
        def _():
            core_copy(lo).wait_send()

        @pl.when(same_send(lo))
        def _():
            loop(lo, nb, lambda i: x_copy(lo, i).wait_send())

    def same_compute(lo):
        slot = lax.rem(lo, RING)

        @pl.when(lo >= RING)
        def _():
            same_drain(lo - RING)

        def one(i):
            far_copy(lo, i).wait()
            last = i == nb - 1

            @pl.when(jnp.logical_or(jnp.logical_not(last), lo < nb - 1))
            def _():
                far_copy(jnp.where(last, lo + 1, lo), jnp.where(last, lo + 1, i + 1)).start()

            part[slot, i] = dot_t(own[i], own[lo]) + dot_t(own[far_slot(lo, i)], own[far_slot(lo, lo)])

        loop(lo, nb, one)

        @pl.when(jnp.logical_not(same))
        def _():
            core_copy(lo).start()

    def same_reduce(lo):
        slot = lax.rem(lo, RING)

        @pl.when(same)
        def _():
            core_copy(lo).wait_recv()
            fetch(got_core.at[lo], other).wait()
            add_other(slot, lo, nb)

        @pl.when(same_send(lo))
        def _():
            loop(lo, nb, lambda i: x_copy(lo, i).start())

    def same_final(lo):
        slot = lax.rem(lo, RING)

        @pl.when(same_recv(lo))
        def _():
            loop(lo, nb, lambda i: x_copy(lo, i).wait_recv())
            fetch(got_x.at[lo], other).wait()
            above = (lax.broadcasted_iota(jnp.int32, (BLOCK, BLOCK), 0)
                     < lax.broadcasted_iota(jnp.int32, (BLOCK, BLOCK), 1))

            def one(i):
                drop = jnp.logical_or(i < lo, jnp.logical_and(i == lo, above))
                cols[pl.ds(pl.multiple_of(i * BLOCK, BLOCK), BLOCK), :] = jnp.where(
                    drop, 0.0, part[slot, i] + other[i]).astype(cols.dtype)

            loop(0, nb, one)
            s = lax.div(lo, 2)
            fetch(cols, out.at[:, pl.ds(pl.multiple_of(s * BLOCK, BLOCK), BLOCK)]).wait()

    first.wait()

    @pl.when(x == 1)
    def _():
        move.wait_recv()

    @pl.when(relays)
    def _():
        relay.start()

    loop(AHEAD, nb, start_a)

    def same_step(t):
        @pl.when(t < nb)
        def _():
            same_compute(t)

        @pl.when(jnp.logical_and(t >= 1, t <= nb))
        def _():
            same_reduce(t - 1)

        @pl.when(t >= 2)
        def _():
            same_final(t - 2)

    loop(0, nb + 2, same_step)

    def mixed_send(b, i):
        split = b + 1 - y
        stay = jnp.logical_and(jnp.logical_not(same), jnp.logical_and(i >= split, lax.rem(b, 2) != x))
        cross = jnp.logical_and(same, jnp.logical_and(i < split, lax.rem(i, 2) != x))
        return jnp.logical_or(stay, cross)

    def mixed_recv(b, i):
        split = b + 1 - y
        stay = jnp.logical_and(jnp.logical_not(same), jnp.logical_and(i >= split, lax.rem(b, 2) == x))
        cross = jnp.logical_and(same, jnp.logical_and(i < split, lax.rem(i, 2) == x))
        return jnp.logical_or(stay, cross)

    def each(cond, action):
        def one(i):
            @pl.when(cond(i))
            def _():
                action(i)

        loop(0, nb, one)

    def mixed_drain(b):
        each(lambda i: mixed_send(b, i), lambda i: x_copy(nb + b, i).wait_send())

    def mixed_reduce(b):
        job = nb + b
        slot = lax.rem(job, RING)
        split = b + 1 - y
        each(lambda i: mixed_recv(b, i), lambda i: x_copy(job, i).wait_recv())
        fetch(got_x.at[job], other).wait()

        @pl.when(jnp.logical_and(jnp.logical_not(same), lax.rem(b, 2) == x))
        def _():
            add_other(slot, split, nb)
            fetch(part.at[slot], kept.at[:, lax.div(b, 2)]).wait()

        @pl.when(same)
        def _():
            def add(i):
                part[slot, i] = part[slot, i] + other[i]

            each(lambda i: mixed_recv(b, i), add)
            fetch(part.at[slot], ready.at[b]).wait()
            each(lambda i: mixed_recv(b, i), lambda i: y_copy(b, i, lambda copy: copy.start()))

    @pl.when(narrow_recv)
    def _():
        own[nb, :, 0:LANES] = jnp.zeros((BLOCK, LANES), own.dtype)

    @pl.when(takes_moved)
    def _():
        relay.wait_recv()
        fetch(moved, extra.at[0]).wait()
        fetch(relayed, extra.at[1]).wait()

    def mixed_step(b):
        job = nb + b
        slot = lax.rem(job, RING)
        split = b + 1 - y

        @pl.when(b < RING)
        def _():
            same_drain(job - RING)

        @pl.when(b >= RING)
        def _():
            mixed_drain(b - RING)

        a_copy(b, narrow_recv, lambda copy: copy.wait_recv())

        @pl.when(narrow_recv)
        def _():
            fetch(got_a.at[b, :, pl.ds(LANES, half - LANES)], own.at[nb, :, pl.ds(LANES, half - LANES)]).wait()

        @pl.when(jnp.logical_not(narrow_recv))
        def _():
            fetch(got_a.at[b], own.at[nb]).wait()

        def one(i):
            lhs = jnp.where(i >= split, i, nb)
            rhs = jnp.where(i >= split, nb, i)
            part[slot, i] = dot_t(own[lhs], own[rhs])

        def one_extra(i):
            left = jnp.where(i >= split, 0, 1)
            part[slot, i] = part[slot, i] + dot_t(extra[left, jnp.where(i >= split, i, b)],
                                                  extra[1 - left, jnp.where(i >= split, b, i)])

        loop(0, nb, one)

        @pl.when(takes_moved)
        def _():
            loop(0, nb, one_extra)

        core_copy(job).start()

        @pl.when(b >= 1)
        def _():
            mixed_reduce(b - 1)

        swap = core_copy(job)
        swap.wait_recv()
        load = fetch(got_core.at[job], other)
        swap.wait_send()
        load.wait()
        add_other(slot, 0, nb)
        each(lambda i: mixed_send(b, i), lambda i: x_copy(job, i).start())

    loop(0, nb, mixed_step)
    mixed_reduce(jnp.int32(nb - 1))

    @pl.when(jnp.logical_not(same))
    def _():
        def wait_y(hi, s):
            @pl.when(2 * s + x < hi + y)
            def _():
                y_copy(hi, 2 * s + x, lambda copy: copy.wait_recv())

        def final(hi):
            mine = fetch(kept.at[hi], other.at[pl.ds(0, cb)], 0)
            loop(0, cb, lambda s: wait_y(hi, s))
            theirs = fetch(got_y.at[hi], other.at[pl.ds(cb, cb)], 1)
            mine.wait()
            theirs.wait()
            for s in range(cb):
                rows[:, s * BLOCK:(s + 1) * BLOCK] = jnp.where(
                    2 * s + x < hi + y, other[s] + other[cb + s], 0.0).astype(rows.dtype)
            fetch(rows, out.at[pl.ds(pl.multiple_of(hi * BLOCK, BLOCK), BLOCK), :]).wait()

        loop(0, nb - 1, final)
        fetch(kept.at[nb - 1], other.at[pl.ds(0, cb)]).wait()
        stores = []
        for s in range(cb):
            wait_y(nb - 1, s)
            span = pl.ds(s * BLOCK, BLOCK)
            rows[:, span] = jnp.where(2 * s + x < nb - 1 + y, other[s] + last_y[s], 0.0).astype(rows.dtype)
            stores.append(fetch(rows.at[:, span], out.at[pl.ds((nb - 1) * BLOCK, BLOCK), span], s))
        for store in stores:
            store.wait()

    def finish(b):
        @pl.when(b >= nb - RING)
        def _():
            mixed_drain(b)

        @pl.when(same)
        def _():
            each(lambda i: mixed_recv(b, i), lambda i: y_copy(b, i, lambda copy: copy.wait_send()))

        a_copy(b, narrow_send, lambda copy: copy.wait_send())

    loop(0, nb, finish)

    @pl.when(x == 0)
    def _():
        move.wait_send()

    @pl.when(relays)
    def _():
        relay.wait_send()


def solution(mesh):
    def local_fn(a_local):
        local_rows, m_local = a_local.shape
        nb = local_rows // BLOCK
        cb = nb // 2
        half = m_local // 2
        f32, bf16 = jnp.float32, a_local.dtype
        hbm = pl.BlockSpec(memory_space=pl.ANY)
        shapes = [
            jax.ShapeDtypeStruct((local_rows, cb * BLOCK), bf16),
            jax.ShapeDtypeStruct((nb, BLOCK, half), bf16),
            jax.ShapeDtypeStruct((2 * nb, nb, BLOCK, BLOCK), f32),
            jax.ShapeDtypeStruct((2 * nb, nb, BLOCK, BLOCK), f32),
            jax.ShapeDtypeStruct((nb, cb, BLOCK, BLOCK), f32),
            jax.ShapeDtypeStruct((nb, cb, BLOCK, BLOCK), f32),
            jax.ShapeDtypeStruct((nb, nb, BLOCK, BLOCK), f32),
            jax.ShapeDtypeStruct((nb, BLOCK, LANES), bf16),
            jax.ShapeDtypeStruct((nb, BLOCK, LANES), bf16),
        ]
        dma = pltpu.SemaphoreType.DMA
        outs = pl.pallas_call(
            kernel,
            out_shape=shapes,
            in_specs=[hbm],
            out_specs=[hbm] * len(shapes),
            scratch_shapes=[
                pltpu.VMEM((nb + 5, BLOCK, half), bf16),
                pltpu.VMEM((RING, nb, BLOCK, BLOCK), f32),
                pltpu.VMEM((nb, BLOCK, BLOCK), f32),
                pltpu.VMEM((local_rows, BLOCK), bf16),
                pltpu.VMEM((BLOCK, cb * BLOCK), bf16),
                pltpu.VMEM((2, nb, BLOCK, LANES), bf16),
                pltpu.VMEM((cb, BLOCK, BLOCK), f32),
                dma((cb,)), dma((4,)),
                dma((nb,)), dma((nb,)),
                dma((RING,)), dma((2 * nb,)),
                dma((RING, nb)), dma((2 * nb, nb)),
                dma((nb, cb)), dma((nb, cb)),
                dma((2,)), dma((2,)),
            ],
            compiler_params=pltpu.CompilerParams(collective_id=0, has_side_effects=True,
                                                 vmem_limit_bytes=46 * 2**20),
            cost_estimate=pl.CostEstimate(flops=210 * 2 * BLOCK * BLOCK * half, bytes_accessed=400 * 2**20,
                                          transcendentals=0),
        )(a_local.reshape(nb, BLOCK, m_local))
        return outs[0]

    part_spec = P(("batch", "row"), "col")
    return jax.shard_map(local_fn, mesh=mesh, in_specs=(part_spec,), out_specs=part_spec, check_vma=False)
```

```python
import functools

import jax
import jax.numpy as jnp
from jax import lax
from jax.experimental import pallas as pl
from jax.experimental.pallas import tpu as pltpu
from jax.sharding import PartitionSpec as P

BLOCK = 256
RING = 3
LANES = 128
AHEAD = 2
MESH = pl.DeviceIdType.MESH
DIMS = (((1,), (1,)), ((), ()))


def dot_t(lhs, rhs):
    return lax.dot_general(lhs, rhs, DIMS, preferred_element_type=jnp.float32)


def loop(lower, upper, body):
    def step(i, carry):
        body(i)
        return carry

    lax.fori_loop(lower, upper, step, 0)


def kernel(a, out, got_a, got_core, got_x, got_y, kept, ready, moved, relayed, own, part, other, cols, rows, extra, last_y,
           load_sem, far_sem, send_a, recv_a, send_core, recv_core, send_x, recv_x, send_y, recv_y, send_m, recv_m):
    nb = a.shape[0]
    cb = nb // 2
    half = a.shape[2] // 2
    y = lax.axis_index("row")
    c = lax.axis_index("col")
    x = lax.div(c, 2)
    k = lax.rem(c, 2)
    same = k == y
    core_dev = {"col": 2 * x + 1 - k}
    x_dev = {"col": 2 * (1 - x) + k}
    y_dev = {"row": 1 - y}

    barrier = pltpu.get_barrier_semaphore()
    for dev in (core_dev, x_dev, y_dev):
        pl.semaphore_signal(barrier, inc=1, device_id=dev, device_id_type=MESH)
    pl.semaphore_wait(barrier, 3)

    def remote(src, dst, send, recv, dev):
        return pltpu.make_async_remote_copy(src_ref=src, dst_ref=dst, send_sem=send, recv_sem=recv,
                                            device_id=dev, device_id_type=MESH)

    def fetch(src, dst, sem=0):
        copy = pltpu.make_async_copy(src, dst, load_sem.at[sem])
        copy.start()
        return copy

    narrow_send = jnp.logical_and(x == 0, y == 0)
    narrow_recv = jnp.logical_and(x == 0, y == 1)
    takes_moved = jnp.logical_and(x == 1, y == 0)
    relays = jnp.logical_and(x == 1, y == 1)

    def wide_copy(b):
        return remote(a.at[b, :, pl.ds(pl.multiple_of((1 - y) * half, half), half)], got_a.at[b],
                      send_a.at[b], recv_a.at[b], y_dev)

    def narrow_copy(b):
        return remote(a.at[b, :, pl.ds(half + LANES, half - LANES)], got_a.at[b, :, pl.ds(LANES, half - LANES)],
                      send_a.at[b], recv_a.at[b], y_dev)

    def a_copy(b, narrow, action):
        @pl.when(narrow)
        def _():
            action(narrow_copy(b))

        @pl.when(jnp.logical_not(narrow))
        def _():
            action(wide_copy(b))

    def start_a(b):
        a_copy(b, narrow_send, lambda copy: copy.start())

    move = remote(a.at[:, :, pl.ds(half, LANES)], moved, send_m.at[0], recv_m.at[0], x_dev)
    relay = remote(moved, relayed, send_m.at[1], recv_m.at[1], y_dev)

    @pl.when(x == 0)
    def _():
        move.start()

    loop(0, AHEAD, start_a)
    first = fetch(a.at[:, :, pl.ds(pl.multiple_of(y * half, half), half)], own.at[pl.ds(0, nb)])

    def far_slot(lo, i):
        return nb + 1 + jnp.where(i == lo, lax.rem(lo, 2), 2 + lax.rem(i, 2))

    def far_copy(lo, i):
        slot = far_slot(lo, i)
        return pltpu.make_async_copy(a.at[i, :, pl.ds(pl.multiple_of((1 - y) * half, half), half)], own.at[slot],
                                     far_sem.at[slot - nb - 1])

    far_copy(jnp.int32(0), jnp.int32(0)).start()

    def core_copy(job, h):
        slot = lax.rem(job, RING)
        span = pl.ds(h * cb, cb)
        return remote(part.at[slot, span], got_core.at[job, span], send_core.at[slot, h], recv_core.at[job, h], core_dev)

    def x_copy(job, i):
        slot = lax.rem(job, RING)
        return remote(part.at[slot, i], got_x.at[job, i], send_x.at[slot, i], recv_x.at[job, i], x_dev)

    def y_copy(b, i, action):
        s = lax.div(i, 2)

        @pl.when(b < nb - 1)
        def _():
            action(remote(ready.at[b, i], got_y.at[b, s], send_y.at[b, s], recv_y.at[b, s], y_dev))

        @pl.when(b == nb - 1)
        def _():
            action(remote(part.at[(2 * nb - 1) % RING, i], last_y.at[s], send_y.at[b, s], recv_y.at[b, s], y_dev))

    def add_other(slot, lower, upper):
        def one(i):
            part[slot, i] = part[slot, i] + other[i]

        loop(lower, upper, one)

    def same_send(lo):
        return jnp.logical_and(same, lax.rem(lo, 2) != x)

    def same_recv(lo):
        return jnp.logical_and(same, lax.rem(lo, 2) == x)

    def same_drain(lo):
        @pl.when(jnp.logical_not(same))
        def _():
            core_copy(lo, 0).wait_send()
            core_copy(lo, 1).wait_send()

        @pl.when(same_send(lo))
        def _():
            loop(lo, nb, lambda i: x_copy(lo, i).wait_send())

    def same_compute(lo):
        slot = lax.rem(lo, RING)

        @pl.when(lo >= RING)
        def _():
            same_drain(lo - RING)

        def one(i):
            far_copy(lo, i).wait()
            last = i == nb - 1

            @pl.when(jnp.logical_or(jnp.logical_not(last), lo < nb - 1))
            def _():
                far_copy(jnp.where(last, lo + 1, lo), jnp.where(last, lo + 1, i + 1)).start()

            part[slot, i] = dot_t(own[i], own[lo]) + dot_t(own[far_slot(lo, i)], own[far_slot(lo, lo)])

        loop(lo, nb, one)

        @pl.when(jnp.logical_not(same))
        def _():
            core_copy(lo, 0).start()
            core_copy(lo, 1).start()

    def same_reduce(lo):
        slot = lax.rem(lo, RING)

        @pl.when(same)
        def _():
            core_copy(lo, 0).wait_recv()
            core_copy(lo, 1).wait_recv()
            fetch(got_core.at[lo], other).wait()
            add_other(slot, lo, nb)

        @pl.when(same_send(lo))
        def _():
            loop(lo, nb, lambda i: x_copy(lo, i).start())

    def same_final(lo):
        slot = lax.rem(lo, RING)

        @pl.when(same_recv(lo))
        def _():
            loop(lo, nb, lambda i: x_copy(lo, i).wait_recv())
            fetch(got_x.at[lo], other).wait()
            above = (lax.broadcasted_iota(jnp.int32, (BLOCK, BLOCK), 0)
                     < lax.broadcasted_iota(jnp.int32, (BLOCK, BLOCK), 1))

            def one(i):
                drop = jnp.logical_or(i < lo, jnp.logical_and(i == lo, above))
                cols[pl.ds(pl.multiple_of(i * BLOCK, BLOCK), BLOCK), :] = jnp.where(
                    drop, 0.0, part[slot, i] + other[i]).astype(cols.dtype)

            loop(0, nb, one)
            s = lax.div(lo, 2)
            fetch(cols, out.at[:, pl.ds(pl.multiple_of(s * BLOCK, BLOCK), BLOCK)]).wait()

    first.wait()

    @pl.when(x == 1)
    def _():
        move.wait_recv()

    @pl.when(relays)
    def _():
        relay.start()

    loop(AHEAD, nb, start_a)

    def same_step(t):
        @pl.when(t < nb)
        def _():
            same_compute(t)

        @pl.when(jnp.logical_and(t >= 1, t <= nb))
        def _():
            same_reduce(t - 1)

        @pl.when(t >= 2)
        def _():
            same_final(t - 2)

    loop(0, nb + 2, same_step)

    def mixed_send(b, i):
        split = b + 1 - y
        stay = jnp.logical_and(jnp.logical_not(same), jnp.logical_and(i >= split, lax.rem(b, 2) != x))
        cross = jnp.logical_and(same, jnp.logical_and(i < split, lax.rem(i, 2) != x))
        return jnp.logical_or(stay, cross)

    def mixed_recv(b, i):
        split = b + 1 - y
        stay = jnp.logical_and(jnp.logical_not(same), jnp.logical_and(i >= split, lax.rem(b, 2) == x))
        cross = jnp.logical_and(same, jnp.logical_and(i < split, lax.rem(i, 2) == x))
        return jnp.logical_or(stay, cross)

    def each(cond, action, lower=0, upper=nb):
        def one(i):
            @pl.when(cond(i))
            def _():
                action(i)

        loop(lower, upper, one)

    def mixed_drain(b):
        each(lambda i: mixed_send(b, i), lambda i: x_copy(nb + b, i).wait_send())

    def mixed_reduce(b):
        job = nb + b
        slot = lax.rem(job, RING)
        split = b + 1 - y
        each(lambda i: mixed_recv(b, i), lambda i: x_copy(job, i).wait_recv())
        fetch(got_x.at[job], other).wait()

        @pl.when(jnp.logical_and(jnp.logical_not(same), lax.rem(b, 2) == x))
        def _():
            add_other(slot, split, nb)
            fetch(part.at[slot], kept.at[:, lax.div(b, 2)]).wait()

        @pl.when(same)
        def _():
            def add(i):
                part[slot, i] = part[slot, i] + other[i]

            each(lambda i: mixed_recv(b, i), add)

            @pl.when(b < nb - 1)
            def _():
                fetch(part.at[slot], ready.at[b]).wait()

            each(lambda i: mixed_recv(b, i), lambda i: y_copy(b, i, lambda copy: copy.start()))

    @pl.when(narrow_recv)
    def _():
        own[nb, :, 0:LANES] = jnp.zeros((BLOCK, LANES), own.dtype)

    @pl.when(takes_moved)
    def _():
        relay.wait_recv()
        fetch(moved, extra.at[0]).wait()
        fetch(relayed, extra.at[1]).wait()

    def mixed_step(b):
        job = nb + b
        slot = lax.rem(job, RING)
        split = b + 1 - y

        @pl.when(b < RING)
        def _():
            same_drain(job - RING)

        @pl.when(b >= RING)
        def _():
            mixed_drain(b - RING)

        early = jnp.logical_and(b >= 1, b <= cb)

        @pl.when(b > cb)
        def _():
            mixed_reduce(b - 1)

        a_copy(b, narrow_recv, lambda copy: copy.wait_recv())

        @pl.when(narrow_recv)
        def _():
            fetch(got_a.at[b, :, pl.ds(LANES, half - LANES)], own.at[nb, :, pl.ds(LANES, half - LANES)]).wait()

        @pl.when(jnp.logical_not(narrow_recv))
        def _():
            fetch(got_a.at[b], own.at[nb]).wait()

        def one(i):
            lhs = jnp.where(i >= split, i, nb)
            rhs = jnp.where(i >= split, nb, i)
            part[slot, i] = dot_t(own[lhs], own[rhs])

        def one_extra(i):
            left = jnp.where(i >= split, 0, 1)
            part[slot, i] = part[slot, i] + dot_t(extra[left, jnp.where(i >= split, i, b)],
                                                  extra[1 - left, jnp.where(i >= split, b, i)])

        def compute_half(h):
            loop(h * cb, h * cb + cb, one)

            @pl.when(takes_moved)
            def _():
                loop(h * cb, h * cb + cb, one_extra)

            core_copy(job, h).start()

        loop(0, 2, compute_half)

        @pl.when(early)
        def _():
            mixed_reduce(b - 1)

        def reduce_half(h):
            swap = core_copy(job, h)
            swap.wait_recv()
            load = fetch(got_core.at[job, pl.ds(h * cb, cb)], other.at[pl.ds(h * cb, cb)])
            swap.wait_send()
            load.wait()
            add_other(slot, h * cb, h * cb + cb)
            each(lambda i: mixed_send(b, i), lambda i: x_copy(job, i).start(), h * cb, h * cb + cb)

        loop(0, 2, reduce_half)

    loop(0, nb, mixed_step)
    mixed_reduce(jnp.int32(nb - 1))

    def finish(b):
        @pl.when(b >= nb - RING)
        def _():
            mixed_drain(b)

        a_copy(b, narrow_send, lambda copy: copy.wait_send())

    loop(0, nb, finish)

    @pl.when(x == 0)
    def _():
        move.wait_send()

    @pl.when(relays)
    def _():
        relay.wait_send()

    @pl.when(jnp.logical_not(same))
    def _():
        def wait_y(hi, s):
            @pl.when(2 * s + x < hi + y)
            def _():
                y_copy(hi, 2 * s + x, lambda copy: copy.wait_recv())

        def final(hi):
            mine = fetch(kept.at[hi], other.at[pl.ds(0, cb)], 0)
            loop(0, cb, lambda s: wait_y(hi, s))
            theirs = fetch(got_y.at[hi], other.at[pl.ds(cb, cb)], 1)
            mine.wait()
            theirs.wait()
            for s in range(cb):
                rows[:, s * BLOCK:(s + 1) * BLOCK] = jnp.where(
                    2 * s + x < hi + y, other[s] + other[cb + s], 0.0).astype(rows.dtype)
            fetch(rows, out.at[pl.ds(pl.multiple_of(hi * BLOCK, BLOCK), BLOCK), :]).wait()

        last_kept = fetch(kept.at[nb - 1], part.at[0, pl.ds(0, cb)], 2)
        loop(0, nb - 1, final)
        last_kept.wait()
        stores = []
        for s in range(cb):
            wait_y(nb - 1, s)
            span = pl.ds(s * BLOCK, BLOCK)
            rows[:, span] = jnp.where(2 * s + x < nb - 1 + y, part[0, s] + last_y[s], 0.0).astype(rows.dtype)
            stores.append(fetch(rows.at[:, span], out.at[pl.ds((nb - 1) * BLOCK, BLOCK), span], s))
        for store in stores:
            store.wait()

    @pl.when(same)
    def _():
        def finish_y(b):
            each(lambda i: mixed_recv(b, i), lambda i: y_copy(b, i, lambda copy: copy.wait_send()))

        loop(0, nb, finish_y)


def solution(mesh):
    def local_fn(a_local):
        local_rows, m_local = a_local.shape
        nb = local_rows // BLOCK
        cb = nb // 2
        half = m_local // 2
        f32, bf16 = jnp.float32, a_local.dtype
        hbm = pl.BlockSpec(memory_space=pl.ANY)
        shapes = [
            jax.ShapeDtypeStruct((local_rows, cb * BLOCK), bf16),
            jax.ShapeDtypeStruct((nb, BLOCK, half), bf16),
            jax.ShapeDtypeStruct((2 * nb, nb, BLOCK, BLOCK), f32),
            jax.ShapeDtypeStruct((2 * nb, nb, BLOCK, BLOCK), f32),
            jax.ShapeDtypeStruct((nb, cb, BLOCK, BLOCK), f32),
            jax.ShapeDtypeStruct((nb, cb, BLOCK, BLOCK), f32),
            jax.ShapeDtypeStruct((nb, nb, BLOCK, BLOCK), f32),
            jax.ShapeDtypeStruct((nb, BLOCK, LANES), bf16),
            jax.ShapeDtypeStruct((nb, BLOCK, LANES), bf16),
        ]
        dma = pltpu.SemaphoreType.DMA
        outs = pl.pallas_call(
            kernel,
            out_shape=shapes,
            in_specs=[hbm],
            out_specs=[hbm] * len(shapes),
            scratch_shapes=[
                pltpu.VMEM((nb + 5, BLOCK, half), bf16),
                pltpu.VMEM((RING, nb, BLOCK, BLOCK), f32),
                pltpu.VMEM((nb, BLOCK, BLOCK), f32),
                pltpu.VMEM((local_rows, BLOCK), bf16),
                pltpu.VMEM((BLOCK, cb * BLOCK), bf16),
                pltpu.VMEM((2, nb, BLOCK, LANES), bf16),
                pltpu.VMEM((cb, BLOCK, BLOCK), f32),
                dma((cb,)), dma((4,)),
                dma((nb,)), dma((nb,)),
                dma((RING, 2)), dma((2 * nb, 2)),
                dma((RING, nb)), dma((2 * nb, nb)),
                dma((nb, cb)), dma((nb, cb)),
                dma((2,)), dma((2,)),
            ],
            compiler_params=pltpu.CompilerParams(collective_id=0, has_side_effects=True,
                                                 vmem_limit_bytes=46 * 2**20),
            cost_estimate=pl.CostEstimate(flops=210 * 2 * BLOCK * BLOCK * half, bytes_accessed=400 * 2**20,
                                          transcendentals=0),
        )(a_local.reshape(nb, BLOCK, m_local))
        return outs[0]

    part_spec = P(("batch", "row"), "col")
    return jax.shard_map(local_fn, mesh=mesh, in_specs=(part_spec,), out_specs=part_spec, check_vma=False)
```

```python
import functools

import jax
import jax.numpy as jnp
from jax import lax
from jax.experimental import pallas as pl
from jax.experimental.pallas import tpu as pltpu
from jax.sharding import PartitionSpec as P

BLOCK = 256
RING = 3
LANES = 128
AHEAD = 2
MESH = pl.DeviceIdType.MESH
DIMS = (((1,), (1,)), ((), ()))


def dot_t(lhs, rhs):
    return lax.dot_general(lhs, rhs, DIMS, preferred_element_type=jnp.float32)


def loop(lower, upper, body):
    def step(i, carry):
        body(i)
        return carry

    lax.fori_loop(lower, upper, step, 0)


def kernel(a, out, got_a, got_core, got_x, got_y, kept, ready, moved, relayed, own, part, other, cols, rows, extra, last_y,
           load_sem, far_sem, send_a, recv_a, send_core, recv_core, send_x, recv_x, send_y, recv_y, send_m, recv_m):
    nb = a.shape[0]
    cb = nb // 2
    half = a.shape[2] // 2
    y = lax.axis_index("row")
    c = lax.axis_index("col")
    x = lax.div(c, 2)
    k = lax.rem(c, 2)
    same = k == y
    core_dev = {"col": 2 * x + 1 - k}
    x_dev = {"col": 2 * (1 - x) + k}
    y_dev = {"row": 1 - y}

    barrier = pltpu.get_barrier_semaphore()
    for dev in (core_dev, x_dev, y_dev):
        pl.semaphore_signal(barrier, inc=1, device_id=dev, device_id_type=MESH)
    pl.semaphore_wait(barrier, 3)

    def remote(src, dst, send, recv, dev):
        return pltpu.make_async_remote_copy(src_ref=src, dst_ref=dst, send_sem=send, recv_sem=recv,
                                            device_id=dev, device_id_type=MESH)

    def fetch(src, dst, sem=0):
        copy = pltpu.make_async_copy(src, dst, load_sem.at[sem])
        copy.start()
        return copy

    narrow_send = jnp.logical_and(x == 0, y == 0)
    narrow_recv = jnp.logical_and(x == 0, y == 1)
    takes_moved = jnp.logical_and(x == 1, y == 0)
    relays = jnp.logical_and(x == 1, y == 1)

    def wide_copy(b):
        return remote(a.at[b, :, pl.ds(pl.multiple_of((1 - y) * half, half), half)], got_a.at[b],
                      send_a.at[b], recv_a.at[b], y_dev)

    def narrow_copy(b):
        return remote(a.at[b, :, pl.ds(half + LANES, half - LANES)], got_a.at[b, :, pl.ds(LANES, half - LANES)],
                      send_a.at[b], recv_a.at[b], y_dev)

    def a_copy(b, narrow, action):
        @pl.when(narrow)
        def _():
            action(narrow_copy(b))

        @pl.when(jnp.logical_not(narrow))
        def _():
            action(wide_copy(b))

    def start_a(b):
        a_copy(b, narrow_send, lambda copy: copy.start())

    move = remote(a.at[:, :, pl.ds(half, LANES)], moved, send_m.at[0], recv_m.at[0], x_dev)
    relay = remote(moved, relayed, send_m.at[1], recv_m.at[1], y_dev)

    @pl.when(x == 0)
    def _():
        move.start()

    loop(0, AHEAD, start_a)
    first = fetch(a.at[:, :, pl.ds(pl.multiple_of(y * half, half), half)], own.at[pl.ds(0, nb)])

    def far_slot(lo, i):
        return nb + 1 + jnp.where(i == lo, lax.rem(lo, 2), 2 + lax.rem(i, 2))

    def far_copy(lo, i):
        slot = far_slot(lo, i)
        return pltpu.make_async_copy(a.at[i, :, pl.ds(pl.multiple_of((1 - y) * half, half), half)], own.at[slot],
                                     far_sem.at[slot - nb - 1])

    far_copy(jnp.int32(0), jnp.int32(0)).start()

    def core_copy(job, h):
        slot = lax.rem(job, RING)
        span = pl.ds(h * cb, cb)
        return remote(part.at[slot, span], got_core.at[job, span], send_core.at[slot, h], recv_core.at[job, h], core_dev)

    def x_copy(job, i):
        slot = lax.rem(job, RING)
        return remote(part.at[slot, i], got_x.at[job, i], send_x.at[slot, i], recv_x.at[job, i], x_dev)

    def y_copy(b, i, action):
        s = lax.div(i, 2)

        @pl.when(b < nb - 1)
        def _():
            action(remote(ready.at[b, i], got_y.at[b, s], send_y.at[b, s], recv_y.at[b, s], y_dev))

        @pl.when(b == nb - 1)
        def _():
            action(remote(part.at[(2 * nb - 1) % RING, i], last_y.at[s], send_y.at[b, s], recv_y.at[b, s], y_dev))

    def add_other(slot, lower, upper):
        def one(i):
            part[slot, i] = part[slot, i] + other[i]

        loop(lower, upper, one)

    def same_send(lo):
        return jnp.logical_and(same, lax.rem(lo, 2) != x)

    def same_recv(lo):
        return jnp.logical_and(same, lax.rem(lo, 2) == x)

    def same_drain(lo):
        @pl.when(jnp.logical_not(same))
        def _():
            core_copy(lo, 0).wait_send()
            core_copy(lo, 1).wait_send()

        @pl.when(same_send(lo))
        def _():
            loop(lo, nb, lambda i: x_copy(lo, i).wait_send())

    def same_compute(lo):
        slot = lax.rem(lo, RING)

        @pl.when(lo >= RING)
        def _():
            same_drain(lo - RING)

        def one(i):
            far_copy(lo, i).wait()
            last = i == nb - 1

            @pl.when(jnp.logical_or(jnp.logical_not(last), lo < nb - 1))
            def _():
                far_copy(jnp.where(last, lo + 1, lo), jnp.where(last, lo + 1, i + 1)).start()

            part[slot, i] = dot_t(own[i], own[lo]) + dot_t(own[far_slot(lo, i)], own[far_slot(lo, lo)])

        loop(lo, nb, one)

        @pl.when(jnp.logical_not(same))
        def _():
            core_copy(lo, 0).start()
            core_copy(lo, 1).start()

    def same_reduce(lo):
        slot = lax.rem(lo, RING)

        @pl.when(same)
        def _():
            core_copy(lo, 0).wait_recv()
            core_copy(lo, 1).wait_recv()
            fetch(got_core.at[lo], other).wait()
            add_other(slot, lo, nb)

        @pl.when(same_send(lo))
        def _():
            loop(lo, nb, lambda i: x_copy(lo, i).start())

    def same_final(lo):
        slot = lax.rem(lo, RING)

        @pl.when(same_recv(lo))
        def _():
            loop(lo, nb, lambda i: x_copy(lo, i).wait_recv())
            fetch(got_x.at[lo], other).wait()
            above = (lax.broadcasted_iota(jnp.int32, (BLOCK, BLOCK), 0)
                     < lax.broadcasted_iota(jnp.int32, (BLOCK, BLOCK), 1))

            def one(i):
                drop = jnp.logical_or(i < lo, jnp.logical_and(i == lo, above))
                cols[pl.ds(pl.multiple_of(i * BLOCK, BLOCK), BLOCK), :] = jnp.where(
                    drop, 0.0, part[slot, i] + other[i]).astype(cols.dtype)

            loop(0, nb, one)
            s = lax.div(lo, 2)
            fetch(cols, out.at[:, pl.ds(pl.multiple_of(s * BLOCK, BLOCK), BLOCK)]).wait()

    first.wait()

    @pl.when(x == 1)
    def _():
        move.wait_recv()

    @pl.when(relays)
    def _():
        relay.start()

    loop(AHEAD, nb, start_a)

    def same_step(t):
        @pl.when(t < nb)
        def _():
            same_compute(t)

        @pl.when(jnp.logical_and(t >= 1, t <= nb))
        def _():
            same_reduce(t - 1)

        @pl.when(t >= 2)
        def _():
            same_final(t - 2)

    loop(0, nb + 2, same_step)

    def mixed_send(b, i):
        split = b + 1 - y
        stay = jnp.logical_and(jnp.logical_not(same), jnp.logical_and(i >= split, lax.rem(b, 2) != x))
        cross = jnp.logical_and(same, jnp.logical_and(i < split, lax.rem(i, 2) != x))
        return jnp.logical_or(stay, cross)

    def mixed_recv(b, i):
        split = b + 1 - y
        stay = jnp.logical_and(jnp.logical_not(same), jnp.logical_and(i >= split, lax.rem(b, 2) == x))
        cross = jnp.logical_and(same, jnp.logical_and(i < split, lax.rem(i, 2) == x))
        return jnp.logical_or(stay, cross)

    def each(cond, action, lower=0, upper=nb):
        def one(i):
            @pl.when(cond(i))
            def _():
                action(i)

        loop(lower, upper, one)

    def mixed_drain(b):
        each(lambda i: mixed_send(b, i), lambda i: x_copy(nb + b, i).wait_send())

    def mixed_reduce(b):
        job = nb + b
        slot = lax.rem(job, RING)
        split = b + 1 - y
        each(lambda i: mixed_recv(b, i), lambda i: x_copy(job, i).wait_recv())
        fetch(got_x.at[job], other).wait()

        @pl.when(jnp.logical_and(jnp.logical_not(same), lax.rem(b, 2) == x))
        def _():
            add_other(slot, split, nb)
            fetch(part.at[slot], kept.at[:, lax.div(b, 2)]).wait()

        @pl.when(same)
        def _():
            def add(i):
                part[slot, i] = part[slot, i] + other[i]

            each(lambda i: mixed_recv(b, i), add)

            @pl.when(b < nb - 1)
            def _():
                fetch(part.at[slot], ready.at[b]).wait()

            each(lambda i: mixed_recv(b, i), lambda i: y_copy(b, i, lambda copy: copy.start()))

    @pl.when(narrow_recv)
    def _():
        own[nb, :, 0:LANES] = jnp.zeros((BLOCK, LANES), own.dtype)

    @pl.when(takes_moved)
    def _():
        relay.wait_recv()
        fetch(moved, extra.at[0]).wait()
        fetch(relayed, extra.at[1]).wait()

    def mixed_step(b):
        job = nb + b
        slot = lax.rem(job, RING)
        split = b + 1 - y

        @pl.when(b < RING)
        def _():
            same_drain(job - RING)

        @pl.when(b >= RING)
        def _():
            mixed_drain(b - RING)

        early = jnp.logical_and(b >= 1, b <= cb)

        @pl.when(b > cb)
        def _():
            mixed_reduce(b - 1)

        a_copy(b, narrow_recv, lambda copy: copy.wait_recv())

        @pl.when(narrow_recv)
        def _():
            fetch(got_a.at[b, :, pl.ds(LANES, half - LANES)], own.at[nb, :, pl.ds(LANES, half - LANES)]).wait()

        @pl.when(jnp.logical_not(narrow_recv))
        def _():
            fetch(got_a.at[b], own.at[nb]).wait()

        def one(i):
            lhs = jnp.where(i >= split, i, nb)
            rhs = jnp.where(i >= split, nb, i)
            part[slot, i] = dot_t(own[lhs], own[rhs])

        def one_extra(i):
            left = jnp.where(i >= split, 0, 1)
            part[slot, i] = part[slot, i] + dot_t(extra[left, jnp.where(i >= split, i, b)],
                                                  extra[1 - left, jnp.where(i >= split, b, i)])

        def compute_half(h):
            loop(h * cb, h * cb + cb, one)

            @pl.when(takes_moved)
            def _():
                loop(h * cb, h * cb + cb, one_extra)

            core_copy(job, h).start()

        loop(0, 2, compute_half)

        @pl.when(early)
        def _():
            mixed_reduce(b - 1)

        def reduce_half(h):
            swap = core_copy(job, h)
            swap.wait_recv()
            load = fetch(got_core.at[job, pl.ds(h * cb, cb)], other.at[pl.ds(h * cb, cb)])
            swap.wait_send()
            load.wait()
            add_other(slot, h * cb, h * cb + cb)
            each(lambda i: mixed_send(b, i), lambda i: x_copy(job, i).start(), h * cb, h * cb + cb)

        loop(0, 2, reduce_half)

    loop(0, nb, mixed_step)
    @pl.when(same)
    def _():
        mixed_reduce(jnp.int32(nb - 1))

    def finish(b):
        @pl.when(b >= nb - RING)
        def _():
            mixed_drain(b)

        a_copy(b, narrow_send, lambda copy: copy.wait_send())

    loop(0, nb, finish)

    @pl.when(x == 0)
    def _():
        move.wait_send()

    @pl.when(relays)
    def _():
        relay.wait_send()

    @pl.when(jnp.logical_not(same))
    def _():
        def wait_y(hi, s):
            @pl.when(2 * s + x < hi + y)
            def _():
                y_copy(hi, 2 * s + x, lambda copy: copy.wait_recv())

        def final(hi):
            mine = fetch(kept.at[hi], other.at[pl.ds(0, cb)], 0)
            loop(0, cb, lambda s: wait_y(hi, s))
            theirs = fetch(got_y.at[hi], other.at[pl.ds(cb, cb)], 1)
            mine.wait()
            theirs.wait()
            for s in range(cb):
                rows[:, s * BLOCK:(s + 1) * BLOCK] = jnp.where(
                    2 * s + x < hi + y, other[s] + other[cb + s], 0.0).astype(rows.dtype)
            fetch(rows, out.at[pl.ds(pl.multiple_of(hi * BLOCK, BLOCK), BLOCK), :]).wait()

        loop(0, nb - 1, final)
        mixed_reduce(jnp.int32(nb - 1))
        fetch(kept.at[nb - 1], part.at[0, pl.ds(0, cb)]).wait()
        stores = []
        for s in range(cb):
            wait_y(nb - 1, s)
            span = pl.ds(s * BLOCK, BLOCK)
            rows[:, span] = jnp.where(2 * s + x < nb - 1 + y, part[0, s] + last_y[s], 0.0).astype(rows.dtype)
            stores.append(fetch(rows.at[:, span], out.at[pl.ds((nb - 1) * BLOCK, BLOCK), span], s))
        for store in stores:
            store.wait()

    @pl.when(same)
    def _():
        def finish_y(b):
            each(lambda i: mixed_recv(b, i), lambda i: y_copy(b, i, lambda copy: copy.wait_send()))

        loop(0, nb, finish_y)


def solution(mesh):
    def local_fn(a_local):
        local_rows, m_local = a_local.shape
        nb = local_rows // BLOCK
        cb = nb // 2
        half = m_local // 2
        f32, bf16 = jnp.float32, a_local.dtype
        hbm = pl.BlockSpec(memory_space=pl.ANY)
        shapes = [
            jax.ShapeDtypeStruct((local_rows, cb * BLOCK), bf16),
            jax.ShapeDtypeStruct((nb, BLOCK, half), bf16),
            jax.ShapeDtypeStruct((2 * nb, nb, BLOCK, BLOCK), f32),
            jax.ShapeDtypeStruct((2 * nb, nb, BLOCK, BLOCK), f32),
            jax.ShapeDtypeStruct((nb, cb, BLOCK, BLOCK), f32),
            jax.ShapeDtypeStruct((nb, cb, BLOCK, BLOCK), f32),
            jax.ShapeDtypeStruct((nb, nb, BLOCK, BLOCK), f32),
            jax.ShapeDtypeStruct((nb, BLOCK, LANES), bf16),
            jax.ShapeDtypeStruct((nb, BLOCK, LANES), bf16),
        ]
        dma = pltpu.SemaphoreType.DMA
        outs = pl.pallas_call(
            kernel,
            out_shape=shapes,
            in_specs=[hbm],
            out_specs=[hbm] * len(shapes),
            scratch_shapes=[
                pltpu.VMEM((nb + 5, BLOCK, half), bf16),
                pltpu.VMEM((RING, nb, BLOCK, BLOCK), f32),
                pltpu.VMEM((nb, BLOCK, BLOCK), f32),
                pltpu.VMEM((local_rows, BLOCK), bf16),
                pltpu.VMEM((BLOCK, cb * BLOCK), bf16),
                pltpu.VMEM((2, nb, BLOCK, LANES), bf16),
                pltpu.VMEM((cb, BLOCK, BLOCK), f32),
                dma((cb,)), dma((4,)),
                dma((nb,)), dma((nb,)),
                dma((RING, 2)), dma((2 * nb, 2)),
                dma((RING, nb)), dma((2 * nb, nb)),
                dma((nb, cb)), dma((nb, cb)),
                dma((2,)), dma((2,)),
            ],
            compiler_params=pltpu.CompilerParams(collective_id=0, has_side_effects=True,
                                                 vmem_limit_bytes=46 * 2**20),
            cost_estimate=pl.CostEstimate(flops=210 * 2 * BLOCK * BLOCK * half, bytes_accessed=400 * 2**20,
                                          transcendentals=0),
        )(a_local.reshape(nb, BLOCK, m_local))
        return outs[0]

    part_spec = P(("batch", "row"), "col")
    return jax.shard_map(local_fn, mesh=mesh, in_specs=(part_spec,), out_specs=part_spec, check_vma=False)
```

```python
import functools

import jax
import jax.numpy as jnp
from jax import lax
from jax.experimental import pallas as pl
from jax.experimental.pallas import tpu as pltpu
from jax.sharding import PartitionSpec as P

BLOCK = 256
RING = 3
LANES = 128
AHEAD = 2
MESH = pl.DeviceIdType.MESH
DIMS = (((1,), (1,)), ((), ()))


def dot_t(lhs, rhs):
    return lax.dot_general(lhs, rhs, DIMS, preferred_element_type=jnp.float32)


def loop(lower, upper, body):
    def step(i, carry):
        body(i)
        return carry

    lax.fori_loop(lower, upper, step, 0)


def kernel(a, out, got_a, got_core, got_x, got_y, kept, ready, moved, relayed, own, part, other, cols, rows, extra, last_y,
           load_sem, far_sem, send_a, recv_a, send_core, recv_core, send_x, recv_x, send_y, recv_y, send_m, recv_m):
    nb = a.shape[0]
    cb = nb // 2
    half = a.shape[2] // 2
    y = lax.axis_index("row")
    c = lax.axis_index("col")
    x = lax.div(c, 2)
    k = lax.rem(c, 2)
    same = k == y
    core_dev = {"col": 2 * x + 1 - k}
    x_dev = {"col": 2 * (1 - x) + k}
    y_dev = {"row": 1 - y}

    barrier = pltpu.get_barrier_semaphore()
    for dev in (core_dev, x_dev, y_dev):
        pl.semaphore_signal(barrier, inc=1, device_id=dev, device_id_type=MESH)
    pl.semaphore_wait(barrier, 3)

    def remote(src, dst, send, recv, dev):
        return pltpu.make_async_remote_copy(src_ref=src, dst_ref=dst, send_sem=send, recv_sem=recv,
                                            device_id=dev, device_id_type=MESH)

    def fetch(src, dst, sem=0):
        copy = pltpu.make_async_copy(src, dst, load_sem.at[sem])
        copy.start()
        return copy

    narrow_send = jnp.logical_and(x == 0, y == 0)
    narrow_recv = jnp.logical_and(x == 0, y == 1)
    takes_moved = jnp.logical_and(x == 1, y == 0)
    relays = jnp.logical_and(x == 1, y == 1)

    def wide_copy(b):
        return remote(a.at[b, :, pl.ds(pl.multiple_of((1 - y) * half, half), half)], got_a.at[b],
                      send_a.at[b], recv_a.at[b], y_dev)

    def narrow_copy(b):
        return remote(a.at[b, :, pl.ds(half + LANES, half - LANES)], got_a.at[b, :, pl.ds(LANES, half - LANES)],
                      send_a.at[b], recv_a.at[b], y_dev)

    def a_copy(b, narrow, action):
        @pl.when(narrow)
        def _():
            action(narrow_copy(b))

        @pl.when(jnp.logical_not(narrow))
        def _():
            action(wide_copy(b))

    def start_a(b):
        a_copy(b, narrow_send, lambda copy: copy.start())

    move = remote(a.at[:, :, pl.ds(half, LANES)], moved, send_m.at[0], recv_m.at[0], x_dev)
    relay = remote(moved, relayed, send_m.at[1], recv_m.at[1], y_dev)

    @pl.when(x == 0)
    def _():
        move.start()

    loop(0, AHEAD, start_a)
    first = fetch(a.at[:, :, pl.ds(pl.multiple_of(y * half, half), half)], own.at[pl.ds(0, nb)])

    def far_slot(lo, i):
        return nb + 1 + jnp.where(i == lo, lax.rem(lo, 2), 2 + lax.rem(i, 2))

    def far_copy(lo, i):
        slot = far_slot(lo, i)
        return pltpu.make_async_copy(a.at[i, :, pl.ds(pl.multiple_of((1 - y) * half, half), half)], own.at[slot],
                                     far_sem.at[slot - nb - 1])

    far_copy(jnp.int32(0), jnp.int32(0)).start()

    def core_copy(job, h):
        slot = lax.rem(job, RING)
        span = pl.ds(h * cb, cb)
        return remote(part.at[slot, span], got_core.at[job, span], send_core.at[slot, h], recv_core.at[job, h], core_dev)

    def x_copy(job, i):
        slot = lax.rem(job, RING)
        return remote(part.at[slot, i], got_x.at[job, i], send_x.at[slot, i], recv_x.at[job, i], x_dev)

    def y_copy(b, i, action):
        s = lax.div(i, 2)

        @pl.when(b < nb - 1)
        def _():
            action(remote(ready.at[b, i], got_y.at[b, s], send_y.at[b, s], recv_y.at[b, s], y_dev))

        @pl.when(b == nb - 1)
        def _():
            action(remote(part.at[(2 * nb - 1) % RING, i], last_y.at[s], send_y.at[b, s], recv_y.at[b, s], y_dev))

    def add_other(slot, lower, upper):
        def one(i):
            part[slot, i] = part[slot, i] + other[i]

        loop(lower, upper, one)

    def same_send(lo):
        return jnp.logical_and(same, lax.rem(lo, 2) != x)

    def same_recv(lo):
        return jnp.logical_and(same, lax.rem(lo, 2) == x)

    def same_drain(lo):
        @pl.when(jnp.logical_not(same))
        def _():
            core_copy(lo, 0).wait_send()
            core_copy(lo, 1).wait_send()

        @pl.when(same_send(lo))
        def _():
            loop(lo, nb, lambda i: x_copy(lo, i).wait_send())

    def same_compute(lo):
        slot = lax.rem(lo, RING)

        @pl.when(lo >= RING)
        def _():
            same_drain(lo - RING)

        def one(i):
            far_copy(lo, i).wait()
            last = i == nb - 1

            @pl.when(jnp.logical_or(jnp.logical_not(last), lo < nb - 1))
            def _():
                far_copy(jnp.where(last, lo + 1, lo), jnp.where(last, lo + 1, i + 1)).start()

            part[slot, i] = dot_t(own[i], own[lo]) + dot_t(own[far_slot(lo, i)], own[far_slot(lo, lo)])

        loop(lo, nb, one)

        @pl.when(jnp.logical_not(same))
        def _():
            core_copy(lo, 0).start()
            core_copy(lo, 1).start()

    def same_reduce(lo):
        slot = lax.rem(lo, RING)

        @pl.when(same)
        def _():
            core_copy(lo, 0).wait_recv()
            core_copy(lo, 1).wait_recv()
            fetch(got_core.at[lo], other).wait()
            add_other(slot, lo, nb)

        @pl.when(same_send(lo))
        def _():
            loop(lo, nb, lambda i: x_copy(lo, i).start())

    def same_final(lo):
        slot = lax.rem(lo, RING)

        @pl.when(same_recv(lo))
        def _():
            loop(lo, nb, lambda i: x_copy(lo, i).wait_recv())
            fetch(got_x.at[lo], other).wait()
            above = (lax.broadcasted_iota(jnp.int32, (BLOCK, BLOCK), 0)
                     < lax.broadcasted_iota(jnp.int32, (BLOCK, BLOCK), 1))

            def one(i):
                drop = jnp.logical_or(i < lo, jnp.logical_and(i == lo, above))
                cols[pl.ds(pl.multiple_of(i * BLOCK, BLOCK), BLOCK), :] = jnp.where(
                    drop, 0.0, part[slot, i] + other[i]).astype(cols.dtype)

            loop(0, nb, one)
            s = lax.div(lo, 2)
            fetch(cols, out.at[:, pl.ds(pl.multiple_of(s * BLOCK, BLOCK), BLOCK)]).wait()

    first.wait()

    @pl.when(x == 1)
    def _():
        move.wait_recv()

    @pl.when(relays)
    def _():
        relay.start()

    loop(AHEAD, nb, start_a)

    def same_step(t):
        @pl.when(t < nb)
        def _():
            same_compute(t)

        @pl.when(jnp.logical_and(t >= 1, t <= nb))
        def _():
            same_reduce(t - 1)

        @pl.when(t >= 2)
        def _():
            same_final(t - 2)

    loop(0, nb + 2, same_step)

    def mixed_send(b, i):
        split = b + 1 - y
        stay = jnp.logical_and(jnp.logical_not(same), jnp.logical_and(i >= split, lax.rem(b, 2) != x))
        cross = jnp.logical_and(same, jnp.logical_and(i < split, lax.rem(i, 2) != x))
        return jnp.logical_or(stay, cross)

    def mixed_recv(b, i):
        split = b + 1 - y
        stay = jnp.logical_and(jnp.logical_not(same), jnp.logical_and(i >= split, lax.rem(b, 2) == x))
        cross = jnp.logical_and(same, jnp.logical_and(i < split, lax.rem(i, 2) == x))
        return jnp.logical_or(stay, cross)

    def each(cond, action, lower=0, upper=nb):
        def one(i):
            @pl.when(cond(i))
            def _():
                action(i)

        loop(lower, upper, one)

    def mixed_drain(b):
        each(lambda i: mixed_send(b, i), lambda i: x_copy(nb + b, i).wait_send())

    def mixed_reduce(b):
        job = nb + b
        slot = lax.rem(job, RING)
        split = b + 1 - y
        each(lambda i: mixed_recv(b, i), lambda i: x_copy(job, i).wait_recv())
        fetch(got_x.at[job], other).wait()

        @pl.when(jnp.logical_and(jnp.logical_not(same), lax.rem(b, 2) == x))
        def _():
            add_other(slot, split, nb)
            fetch(part.at[slot], kept.at[:, lax.div(b, 2)]).wait()

        @pl.when(same)
        def _():
            def add(i):
                part[slot, i] = part[slot, i] + other[i]

            each(lambda i: mixed_recv(b, i), add)

            @pl.when(b < nb - 1)
            def _():
                fetch(part.at[slot], ready.at[b]).wait()

            each(lambda i: mixed_recv(b, i), lambda i: y_copy(b, i, lambda copy: copy.start()))

    @pl.when(narrow_recv)
    def _():
        own[nb, :, 0:LANES] = jnp.zeros((BLOCK, LANES), own.dtype)

    @pl.when(takes_moved)
    def _():
        relay.wait_recv()
        fetch(moved, extra.at[0]).wait()
        fetch(relayed, extra.at[1]).wait()

    def mixed_step(b):
        job = nb + b
        slot = lax.rem(job, RING)
        split = b + 1 - y

        @pl.when(b < RING)
        def _():
            same_drain(job - RING)

        @pl.when(b >= RING)
        def _():
            mixed_drain(b - RING)

        early = jnp.logical_and(b >= 1, b <= cb)

        @pl.when(b > cb)
        def _():
            mixed_reduce(b - 1)

        a_copy(b, narrow_recv, lambda copy: copy.wait_recv())

        @pl.when(narrow_recv)
        def _():
            fetch(got_a.at[b, :, pl.ds(LANES, half - LANES)], own.at[nb, :, pl.ds(LANES, half - LANES)]).wait()

        @pl.when(jnp.logical_not(narrow_recv))
        def _():
            fetch(got_a.at[b], own.at[nb]).wait()

        def one(i):
            lhs = jnp.where(i >= split, i, nb)
            rhs = jnp.where(i >= split, nb, i)
            part[slot, i] = dot_t(own[lhs], own[rhs])

        def one_extra(i):
            left = jnp.where(i >= split, 0, 1)
            part[slot, i] = part[slot, i] + dot_t(extra[left, jnp.where(i >= split, i, b)],
                                                  extra[1 - left, jnp.where(i >= split, b, i)])

        def compute_half(h):
            loop(h * cb, h * cb + cb, one)

            @pl.when(takes_moved)
            def _():
                loop(h * cb, h * cb + cb, one_extra)

            core_copy(job, h).start()

        loop(0, 2, compute_half)

        @pl.when(early)
        def _():
            mixed_reduce(b - 1)

        def reduce_half(h):
            swap = core_copy(job, h)
            swap.wait_recv()
            load = fetch(got_core.at[job, pl.ds(h * cb, cb)], other.at[pl.ds(h * cb, cb)])
            swap.wait_send()
            load.wait()
            add_other(slot, h * cb, h * cb + cb)
            each(lambda i: mixed_send(b, i), lambda i: x_copy(job, i).start(), h * cb, h * cb + cb)

        loop(0, 2, reduce_half)

    loop(0, nb, mixed_step)
    @pl.when(same)
    def _():
        mixed_reduce(jnp.int32(nb - 1))

    def finish(b):
        @pl.when(b >= nb - RING)
        def _():
            mixed_drain(b)

        a_copy(b, narrow_send, lambda copy: copy.wait_send())

    loop(0, nb, finish)

    @pl.when(x == 0)
    def _():
        move.wait_send()

    @pl.when(relays)
    def _():
        relay.wait_send()

    @pl.when(jnp.logical_not(same))
    def _():
        def wait_y(hi, s):
            @pl.when(2 * s + x < hi + y)
            def _():
                y_copy(hi, 2 * s + x, lambda copy: copy.wait_recv())

        def final(hi):
            mine = fetch(kept.at[hi], other.at[pl.ds(0, cb)], 0)
            loop(0, cb, lambda s: wait_y(hi, s))
            theirs = fetch(got_y.at[hi], other.at[pl.ds(cb, cb)], 1)
            mine.wait()
            theirs.wait()
            for s in range(cb):
                rows[:, s * BLOCK:(s + 1) * BLOCK] = jnp.where(
                    2 * s + x < hi + y, other[s] + other[cb + s], 0.0).astype(rows.dtype)
            fetch(rows, out.at[pl.ds(pl.multiple_of(hi * BLOCK, BLOCK), BLOCK), :]).wait()

        loop(0, nb - 1, final)
        mixed_reduce(jnp.int32(nb - 1))
        fetch(kept.at[nb - 1], part.at[0, pl.ds(0, cb)]).wait()
        stores = []
        for s in range(cb):
            wait_y(nb - 1, s)
            span = pl.ds(s * BLOCK, BLOCK)
            rows[:, span] = jnp.where(2 * s + x < nb - 1 + y, part[0, s] + last_y[s], 0.0).astype(rows.dtype)
            stores.append(fetch(rows.at[:, span], out.at[pl.ds((nb - 1) * BLOCK, BLOCK), span], s))
        for store in stores:
            store.wait()

    @pl.when(same)
    def _():
        def finish_y(b):
            each(lambda i: mixed_recv(b, i), lambda i: y_copy(b, i, lambda copy: copy.wait_send()))

        loop(0, nb, finish_y)


def store(src, out, sem):
    parts = sem.shape[0]
    size = src.shape[0] // parts
    copies = [pltpu.make_async_copy(src.at[pl.ds(p * size, size)], out.at[pl.ds(p * size, size)], sem.at[p])
              for p in range(parts)]
    for copy in copies:
        copy.start()
    for copy in copies:
        copy.wait()


def solution(mesh):
    def local_fn(a_local):
        local_rows, m_local = a_local.shape
        nb = local_rows // BLOCK
        cb = nb // 2
        half = m_local // 2
        f32, bf16 = jnp.float32, a_local.dtype
        hbm = pl.BlockSpec(memory_space=pl.ANY)
        shapes = [
            jax.ShapeDtypeStruct((local_rows, cb * BLOCK), bf16),
            jax.ShapeDtypeStruct((nb, BLOCK, half), bf16),
            jax.ShapeDtypeStruct((2 * nb, nb, BLOCK, BLOCK), f32),
            jax.ShapeDtypeStruct((2 * nb, nb, BLOCK, BLOCK), f32),
            jax.ShapeDtypeStruct((nb, cb, BLOCK, BLOCK), f32),
            jax.ShapeDtypeStruct((nb, cb, BLOCK, BLOCK), f32),
            jax.ShapeDtypeStruct((nb, nb, BLOCK, BLOCK), f32),
            jax.ShapeDtypeStruct((nb, BLOCK, LANES), bf16),
            jax.ShapeDtypeStruct((nb, BLOCK, LANES), bf16),
        ]
        dma = pltpu.SemaphoreType.DMA
        outs = pl.pallas_call(
            kernel,
            out_shape=shapes,
            in_specs=[hbm],
            out_specs=[hbm] * len(shapes),
            scratch_shapes=[
                pltpu.VMEM((nb + 5, BLOCK, half), bf16),
                pltpu.VMEM((RING, nb, BLOCK, BLOCK), f32),
                pltpu.VMEM((nb, BLOCK, BLOCK), f32),
                pltpu.VMEM((local_rows, BLOCK), bf16),
                pltpu.VMEM((BLOCK, cb * BLOCK), bf16),
                pltpu.VMEM((2, nb, BLOCK, LANES), bf16),
                pltpu.VMEM((cb, BLOCK, BLOCK), f32),
                dma((cb,)), dma((4,)),
                dma((nb,)), dma((nb,)),
                dma((RING, 2)), dma((2 * nb, 2)),
                dma((RING, nb)), dma((2 * nb, nb)),
                dma((nb, cb)), dma((nb, cb)),
                dma((2,)), dma((2,)),
            ],
            compiler_params=pltpu.CompilerParams(collective_id=0, has_side_effects=True,
                                                 vmem_limit_bytes=46 * 2**20),
            cost_estimate=pl.CostEstimate(flops=210 * 2 * BLOCK * BLOCK * half, bytes_accessed=400 * 2**20,
                                          transcendentals=0),
        )(a_local.reshape(nb, BLOCK, m_local))
        return pl.pallas_call(
            store,
            out_shape=shapes[0],
            in_specs=[hbm],
            out_specs=hbm,
            scratch_shapes=[dma((4,))],
            compiler_params=pltpu.CompilerParams(vmem_limit_bytes=2**20),
            cost_estimate=pl.CostEstimate(flops=0, bytes_accessed=2 * shapes[0].size * 2, transcendentals=0),
        )(outs[0])

    part_spec = P(("batch", "row"), "col")
    return jax.shard_map(local_fn, mesh=mesh, in_specs=(part_spec,), out_specs=part_spec, check_vma=False)
```

```python
import functools

import jax
import jax.numpy as jnp
from jax import lax
from jax.experimental import pallas as pl
from jax.experimental.pallas import tpu as pltpu
from jax.sharding import PartitionSpec as P

BLOCK = 256
RING = 3
LANES = 128
AHEAD = 2
MESH = pl.DeviceIdType.MESH
DIMS = (((1,), (1,)), ((), ()))


def dot_t(lhs, rhs):
    return lax.dot_general(lhs, rhs, DIMS, preferred_element_type=jnp.float32)


def loop(lower, upper, body):
    def step(i, carry):
        body(i)
        return carry

    lax.fori_loop(lower, upper, step, 0)


def kernel(a, out, got_a, got_core, got_x, got_y, kept, ready, moved, relayed, own, part, other, cols, extra, last_y,
           load_sem, far_sem, send_a, recv_a, send_core, recv_core, send_x, recv_x, send_y, recv_y, send_m, recv_m):
    nb = a.shape[0]
    cb = nb // 2
    half = a.shape[2] // 2
    y = lax.axis_index("row")
    c = lax.axis_index("col")
    x = lax.div(c, 2)
    k = lax.rem(c, 2)
    same = k == y
    core_dev = {"col": 2 * x + 1 - k}
    x_dev = {"col": 2 * (1 - x) + k}
    y_dev = {"row": 1 - y}

    barrier = pltpu.get_barrier_semaphore()
    for dev in (core_dev, x_dev, y_dev):
        pl.semaphore_signal(barrier, inc=1, device_id=dev, device_id_type=MESH)
    pl.semaphore_wait(barrier, 3)

    def remote(src, dst, send, recv, dev):
        return pltpu.make_async_remote_copy(src_ref=src, dst_ref=dst, send_sem=send, recv_sem=recv,
                                            device_id=dev, device_id_type=MESH)

    def fetch(src, dst, sem=0):
        copy = pltpu.make_async_copy(src, dst, load_sem.at[sem])
        copy.start()
        return copy

    narrow_send = jnp.logical_and(x == 0, y == 0)
    narrow_recv = jnp.logical_and(x == 0, y == 1)
    takes_moved = jnp.logical_and(x == 1, y == 0)
    relays = jnp.logical_and(x == 1, y == 1)

    def wide_copy(b):
        return remote(a.at[b, :, pl.ds(pl.multiple_of((1 - y) * half, half), half)], got_a.at[b],
                      send_a.at[b], recv_a.at[b], y_dev)

    def narrow_copy(b):
        return remote(a.at[b, :, pl.ds(half + LANES, half - LANES)], got_a.at[b, :, pl.ds(LANES, half - LANES)],
                      send_a.at[b], recv_a.at[b], y_dev)

    def a_copy(b, narrow, action):
        @pl.when(narrow)
        def _():
            action(narrow_copy(b))

        @pl.when(jnp.logical_not(narrow))
        def _():
            action(wide_copy(b))

    def start_a(b):
        a_copy(b, narrow_send, lambda copy: copy.start())

    move = remote(a.at[:, :, pl.ds(half, LANES)], moved, send_m.at[0], recv_m.at[0], x_dev)
    relay = remote(moved, relayed, send_m.at[1], recv_m.at[1], y_dev)

    @pl.when(x == 0)
    def _():
        move.start()

    loop(0, AHEAD, start_a)
    first = fetch(a.at[:, :, pl.ds(pl.multiple_of(y * half, half), half)], own.at[pl.ds(0, nb)])

    def far_slot(lo, i):
        count = lo * (nb - 1) - lax.div(lo * (lo - 1), 2) + i - lo - 1
        return nb + 1 + jnp.where(i == lo, lax.rem(lo, 2), 2 + lax.rem(jnp.maximum(count, 0), 3))

    def far_next(lo, i):
        last = i == nb - 1
        return jnp.where(last, lo + 1, lo), jnp.where(last, lo + 1, i + 1)

    def far_copy(lo, i):
        slot = far_slot(lo, i)
        return pltpu.make_async_copy(a.at[i, :, pl.ds(pl.multiple_of((1 - y) * half, half), half)], own.at[slot],
                                     far_sem.at[slot - nb - 1])

    far_copy(jnp.int32(0), jnp.int32(0)).start()
    far_copy(jnp.int32(0), jnp.int32(1)).start()

    def core_copy(job, h):
        slot = lax.rem(job, RING)
        span = pl.ds(h * cb, cb)
        return remote(part.at[slot, span], got_core.at[job, span], send_core.at[slot, h], recv_core.at[job, h], core_dev)

    def x_copy(job, i):
        slot = lax.rem(job, RING)
        return remote(part.at[slot, i], got_x.at[job, i], send_x.at[slot, i], recv_x.at[job, i], x_dev)

    def y_copy(b, i, action):
        s = lax.div(i, 2)

        @pl.when(b < nb - 1)
        def _():
            action(remote(ready.at[b, i], got_y.at[b, s], send_y.at[b, s], recv_y.at[b, s], y_dev))

        @pl.when(b == nb - 1)
        def _():
            action(remote(part.at[(2 * nb - 1) % RING, i], last_y.at[s], send_y.at[b, s], recv_y.at[b, s], y_dev))

    def add_other(slot, lower, upper):
        def one(i):
            part[slot, i] = part[slot, i] + other[i]

        loop(lower, upper, one)

    def same_send(lo):
        return jnp.logical_and(same, lax.rem(lo, 2) != x)

    def same_recv(lo):
        return jnp.logical_and(same, lax.rem(lo, 2) == x)

    def same_drain(lo):
        @pl.when(jnp.logical_not(same))
        def _():
            core_copy(lo, 0).wait_send()
            core_copy(lo, 1).wait_send()

        @pl.when(same_send(lo))
        def _():
            loop(lo, nb, lambda i: x_copy(lo, i).wait_send())

    def same_compute(lo):
        slot = lax.rem(lo, RING)

        @pl.when(lo >= RING)
        def _():
            same_drain(lo - RING)

        def one(i):
            far_copy(lo, i).wait()
            ahead = far_next(*far_next(lo, i))

            @pl.when(ahead[0] < nb)
            def _():
                far_copy(*ahead).start()

            part[slot, i] = dot_t(own[i], own[lo]) + dot_t(own[far_slot(lo, i)], own[far_slot(lo, lo)])

        loop(lo, nb, one)

        @pl.when(jnp.logical_not(same))
        def _():
            core_copy(lo, 0).start()
            core_copy(lo, 1).start()

    def same_reduce(lo):
        slot = lax.rem(lo, RING)

        @pl.when(same)
        def _():
            core_copy(lo, 0).wait_recv()
            core_copy(lo, 1).wait_recv()
            fetch(got_core.at[lo], other).wait()
            add_other(slot, lo, nb)

        @pl.when(same_send(lo))
        def _():
            loop(lo, nb, lambda i: x_copy(lo, i).start())

    def same_final(lo):
        slot = lax.rem(lo, RING)

        @pl.when(same_recv(lo))
        def _():
            loop(lo, nb, lambda i: x_copy(lo, i).wait_recv())
            fetch(got_x.at[lo], other).wait()
            above = (lax.broadcasted_iota(jnp.int32, (BLOCK, BLOCK), 0)
                     < lax.broadcasted_iota(jnp.int32, (BLOCK, BLOCK), 1))

            def one(i):
                drop = jnp.logical_or(i < lo, jnp.logical_and(i == lo, above))
                cols[pl.ds(pl.multiple_of(i * BLOCK, BLOCK), BLOCK), :] = jnp.where(
                    drop, 0.0, part[slot, i] + other[i]).astype(cols.dtype)

            loop(0, nb, one)
            s = lax.div(lo, 2)
            fetch(cols, out.at[:, pl.ds(pl.multiple_of(s * BLOCK, BLOCK), BLOCK)]).wait()

    first.wait()

    @pl.when(x == 1)
    def _():
        move.wait_recv()

    @pl.when(relays)
    def _():
        relay.start()

    loop(AHEAD, nb, start_a)

    def same_step(t):
        @pl.when(t < nb)
        def _():
            same_compute(t)

        @pl.when(jnp.logical_and(t >= 1, t <= nb))
        def _():
            same_reduce(t - 1)

        @pl.when(t >= 2)
        def _():
            same_final(t - 2)

    loop(0, nb + 2, same_step)

    def mixed_send(b, i):
        split = b + 1 - y
        stay = jnp.logical_and(jnp.logical_not(same), jnp.logical_and(i >= split, lax.rem(b, 2) != x))
        cross = jnp.logical_and(same, jnp.logical_and(i < split, lax.rem(i, 2) != x))
        return jnp.logical_or(stay, cross)

    def mixed_recv(b, i):
        split = b + 1 - y
        stay = jnp.logical_and(jnp.logical_not(same), jnp.logical_and(i >= split, lax.rem(b, 2) == x))
        cross = jnp.logical_and(same, jnp.logical_and(i < split, lax.rem(i, 2) == x))
        return jnp.logical_or(stay, cross)

    def each(cond, action, lower=0, upper=nb):
        def one(i):
            @pl.when(cond(i))
            def _():
                action(i)

        loop(lower, upper, one)

    def mixed_drain(b):
        each(lambda i: mixed_send(b, i), lambda i: x_copy(nb + b, i).wait_send())

    def mixed_reduce(b):
        job = nb + b
        slot = lax.rem(job, RING)
        split = b + 1 - y
        each(lambda i: mixed_recv(b, i), lambda i: x_copy(job, i).wait_recv())
        fetch(got_x.at[job], other).wait()

        @pl.when(jnp.logical_and(jnp.logical_not(same), lax.rem(b, 2) == x))
        def _():
            add_other(slot, split, nb)
            fetch(part.at[slot], kept.at[:, lax.div(b, 2)]).wait()

        @pl.when(same)
        def _():
            def add(i):
                part[slot, i] = part[slot, i] + other[i]

            each(lambda i: mixed_recv(b, i), add)

            @pl.when(b < nb - 1)
            def _():
                fetch(part.at[slot], ready.at[b]).wait()

            each(lambda i: mixed_recv(b, i), lambda i: y_copy(b, i, lambda copy: copy.start()))

    @pl.when(narrow_recv)
    def _():
        own[nb, :, 0:LANES] = jnp.zeros((BLOCK, LANES), own.dtype)

    @pl.when(takes_moved)
    def _():
        relay.wait_recv()
        fetch(moved, extra.at[0]).wait()
        fetch(relayed, extra.at[1]).wait()

    def mixed_step(b):
        job = nb + b
        slot = lax.rem(job, RING)
        split = b + 1 - y

        @pl.when(b < RING)
        def _():
            same_drain(job - RING)

        @pl.when(b >= RING)
        def _():
            mixed_drain(b - RING)

        early = jnp.logical_and(b >= 1, b <= cb)

        @pl.when(b > cb)
        def _():
            mixed_reduce(b - 1)

        a_copy(b, narrow_recv, lambda copy: copy.wait_recv())

        @pl.when(narrow_recv)
        def _():
            fetch(got_a.at[b, :, pl.ds(LANES, half - LANES)], own.at[nb, :, pl.ds(LANES, half - LANES)]).wait()

        @pl.when(jnp.logical_not(narrow_recv))
        def _():
            fetch(got_a.at[b], own.at[nb]).wait()

        def one(i):
            lhs = jnp.where(i >= split, i, nb)
            rhs = jnp.where(i >= split, nb, i)
            part[slot, i] = dot_t(own[lhs], own[rhs])

        def one_extra(i):
            left = jnp.where(i >= split, 0, 1)
            part[slot, i] = part[slot, i] + dot_t(extra[left, jnp.where(i >= split, i, b)],
                                                  extra[1 - left, jnp.where(i >= split, b, i)])

        def compute_half(h):
            loop(h * cb, h * cb + cb, one)

            @pl.when(takes_moved)
            def _():
                loop(h * cb, h * cb + cb, one_extra)

            core_copy(job, h).start()

        loop(0, 2, compute_half)

        @pl.when(early)
        def _():
            mixed_reduce(b - 1)

        def reduce_half(h):
            swap = core_copy(job, h)
            swap.wait_recv()
            load = fetch(got_core.at[job, pl.ds(h * cb, cb)], other.at[pl.ds(h * cb, cb)])
            swap.wait_send()
            load.wait()
            add_other(slot, h * cb, h * cb + cb)
            each(lambda i: mixed_send(b, i), lambda i: x_copy(job, i).start(), h * cb, h * cb + cb)

        loop(0, 2, reduce_half)

    loop(0, nb, mixed_step)
    @pl.when(same)
    def _():
        mixed_reduce(jnp.int32(nb - 1))

    def finish(b):
        @pl.when(b >= nb - RING)
        def _():
            mixed_drain(b)

        a_copy(b, narrow_send, lambda copy: copy.wait_send())

    loop(0, nb, finish)

    @pl.when(x == 0)
    def _():
        move.wait_send()

    @pl.when(relays)
    def _():
        relay.wait_send()

    @pl.when(jnp.logical_not(same))
    def _():
        def wait_y(hi, s):
            @pl.when(2 * s + x < hi + y)
            def _():
                y_copy(hi, 2 * s + x, lambda copy: copy.wait_recv())

        def store_block(hi, s):
            span = pl.ds(s * BLOCK, BLOCK)
            return fetch(cols.at[span], out.at[pl.ds(pl.multiple_of(hi * BLOCK, BLOCK), BLOCK), span], s)

        def final(hi):
            mine = fetch(kept.at[hi], other.at[pl.ds(0, cb)], 0)
            loop(0, cb, lambda s: wait_y(hi, s))
            theirs = fetch(got_y.at[hi], other.at[pl.ds(cb, cb)], 1)
            mine.wait()
            theirs.wait()
            stores = []
            for s in range(cb):
                cols[s * BLOCK:(s + 1) * BLOCK, :] = jnp.where(
                    2 * s + x < hi + y, other[s] + other[cb + s], 0.0).astype(cols.dtype)
                stores.append(store_block(hi, s))
            for store in stores:
                store.wait()

        loop(0, nb - 1, final)
        mixed_reduce(jnp.int32(nb - 1))
        fetch(kept.at[nb - 1], part.at[0, pl.ds(0, cb)]).wait()
        stores = []
        for s in range(cb):
            wait_y(nb - 1, s)
            cols[s * BLOCK:(s + 1) * BLOCK, :] = jnp.where(
                2 * s + x < nb - 1 + y, part[0, s] + last_y[s], 0.0).astype(cols.dtype)
            stores.append(store_block(nb - 1, s))
        for store in stores:
            store.wait()

    @pl.when(same)
    def _():
        def finish_y(b):
            each(lambda i: mixed_recv(b, i), lambda i: y_copy(b, i, lambda copy: copy.wait_send()))

        loop(0, nb, finish_y)


def solution(mesh):
    def local_fn(a_local):
        local_rows, m_local = a_local.shape
        nb = local_rows // BLOCK
        cb = nb // 2
        half = m_local // 2
        f32, bf16 = jnp.float32, a_local.dtype
        hbm = pl.BlockSpec(memory_space=pl.ANY)
        shapes = [
            jax.ShapeDtypeStruct((local_rows, cb * BLOCK), bf16),
            jax.ShapeDtypeStruct((nb, BLOCK, half), bf16),
            jax.ShapeDtypeStruct((2 * nb, nb, BLOCK, BLOCK), f32),
            jax.ShapeDtypeStruct((2 * nb, nb, BLOCK, BLOCK), f32),
            jax.ShapeDtypeStruct((nb, cb, BLOCK, BLOCK), f32),
            jax.ShapeDtypeStruct((nb, cb, BLOCK, BLOCK), f32),
            jax.ShapeDtypeStruct((nb, nb, BLOCK, BLOCK), f32),
            jax.ShapeDtypeStruct((nb, BLOCK, LANES), bf16),
            jax.ShapeDtypeStruct((nb, BLOCK, LANES), bf16),
        ]
        dma = pltpu.SemaphoreType.DMA
        outs = pl.pallas_call(
            kernel,
            out_shape=shapes,
            in_specs=[hbm],
            out_specs=[hbm] * len(shapes),
            scratch_shapes=[
                pltpu.VMEM((nb + 6, BLOCK, half), bf16),
                pltpu.VMEM((RING, nb, BLOCK, BLOCK), f32),
                pltpu.VMEM((nb, BLOCK, BLOCK), f32),
                pltpu.VMEM((local_rows, BLOCK), bf16),
                pltpu.VMEM((2, nb, BLOCK, LANES), bf16),
                pltpu.VMEM((cb, BLOCK, BLOCK), f32),
                dma((cb,)), dma((5,)),
                dma((nb,)), dma((nb,)),
                dma((RING, 2)), dma((2 * nb, 2)),
                dma((RING, nb)), dma((2 * nb, nb)),
                dma((nb, cb)), dma((nb, cb)),
                dma((2,)), dma((2,)),
            ],
            compiler_params=pltpu.CompilerParams(collective_id=0, has_side_effects=True,
                                                 vmem_limit_bytes=46 * 2**20),
            cost_estimate=pl.CostEstimate(flops=210 * 2 * BLOCK * BLOCK * half, bytes_accessed=400 * 2**20,
                                          transcendentals=0),
        )(a_local.reshape(nb, BLOCK, m_local))
        return outs[0]

    part_spec = P(("batch", "row"), "col")
    return jax.shard_map(local_fn, mesh=mesh, in_specs=(part_spec,), out_specs=part_spec, check_vma=False)
```

```python
import functools

import jax
import jax.numpy as jnp
from jax import lax
from jax.experimental import pallas as pl
from jax.experimental.pallas import tpu as pltpu
from jax.sharding import PartitionSpec as P

BLOCK = 256
RING = 3
LANES = 128
AHEAD = 2
MESH = pl.DeviceIdType.MESH
DIMS = (((1,), (1,)), ((), ()))


def dot_t(lhs, rhs):
    return lax.dot_general(lhs, rhs, DIMS, preferred_element_type=jnp.float32)


def loop(lower, upper, body):
    def step(i, carry):
        body(i)
        return carry

    lax.fori_loop(lower, upper, step, 0)


def kernel(a, out, got_a, got_core, got_x, got_y, kept, ready, moved, relayed, own, part, other, cols, extra,
           load_sem, far_sem, send_a, recv_a, send_core, recv_core, send_x, recv_x, send_y, recv_y, send_m, recv_m):
    nb = a.shape[0]
    cb = nb // 2
    half = a.shape[2] // 2
    y = lax.axis_index("row")
    c = lax.axis_index("col")
    x = lax.div(c, 2)
    k = lax.rem(c, 2)
    same = k == y
    core_dev = {"col": 2 * x + 1 - k}
    x_dev = {"col": 2 * (1 - x) + k}
    y_dev = {"row": 1 - y}

    barrier = pltpu.get_barrier_semaphore()
    for dev in (core_dev, x_dev, y_dev):
        pl.semaphore_signal(barrier, inc=1, device_id=dev, device_id_type=MESH)
    pl.semaphore_wait(barrier, 3)

    def remote(src, dst, send, recv, dev):
        return pltpu.make_async_remote_copy(src_ref=src, dst_ref=dst, send_sem=send, recv_sem=recv,
                                            device_id=dev, device_id_type=MESH)

    def fetch(src, dst, sem=0):
        copy = pltpu.make_async_copy(src, dst, load_sem.at[sem])
        copy.start()
        return copy

    narrow_send = jnp.logical_and(x == 0, y == 0)
    narrow_recv = jnp.logical_and(x == 0, y == 1)
    takes_moved = jnp.logical_and(x == 1, y == 0)
    relays = jnp.logical_and(x == 1, y == 1)

    def wide_copy(b):
        return remote(a.at[b, :, pl.ds(pl.multiple_of((1 - y) * half, half), half)], got_a.at[b],
                      send_a.at[b], recv_a.at[b], y_dev)

    def narrow_copy(b):
        return remote(a.at[b, :, pl.ds(half + LANES, half - LANES)], got_a.at[b, :, pl.ds(LANES, half - LANES)],
                      send_a.at[b], recv_a.at[b], y_dev)

    def a_copy(b, narrow, action):
        @pl.when(narrow)
        def _():
            action(narrow_copy(b))

        @pl.when(jnp.logical_not(narrow))
        def _():
            action(wide_copy(b))

    def start_a(b):
        a_copy(b, narrow_send, lambda copy: copy.start())

    move = remote(a.at[:, :, pl.ds(half, LANES)], moved, send_m.at[0], recv_m.at[0], x_dev)
    relay = remote(moved, relayed, send_m.at[1], recv_m.at[1], y_dev)

    @pl.when(x == 0)
    def _():
        move.start()

    loop(0, AHEAD, start_a)
    first = fetch(a.at[:, :, pl.ds(pl.multiple_of(y * half, half), half)], own.at[pl.ds(0, nb)])

    def far_slot(lo, i):
        count = lo * (nb - 1) - lax.div(lo * (lo - 1), 2) + i - lo - 1
        return nb + 1 + jnp.where(i == lo, lax.rem(lo, 2), 2 + lax.rem(jnp.maximum(count, 0), 3))

    def far_next(lo, i):
        last = i == nb - 1
        return jnp.where(last, lo + 1, lo), jnp.where(last, lo + 1, i + 1)

    def far_copy(lo, i):
        slot = far_slot(lo, i)
        return pltpu.make_async_copy(a.at[i, :, pl.ds(pl.multiple_of((1 - y) * half, half), half)], own.at[slot],
                                     far_sem.at[slot - nb - 1])

    far_copy(jnp.int32(0), jnp.int32(0)).start()
    far_copy(jnp.int32(0), jnp.int32(1)).start()

    def core_copy(job, h):
        slot = lax.rem(job, RING)
        span = pl.ds(h * cb, cb)
        return remote(part.at[slot, span], got_core.at[job, span], send_core.at[slot, h], recv_core.at[job, h], core_dev)

    def x_copy(job, i):
        slot = lax.rem(job, RING)
        return remote(part.at[slot, i], got_x.at[job, i], send_x.at[slot, i], recv_x.at[job, i], x_dev)

    def y_copy(b, i, action):
        s = lax.div(i, 2)

        @pl.when(b < nb - 1)
        def _():
            action(remote(ready.at[b, i], got_y.at[b, s], send_y.at[b, s], recv_y.at[b, s], y_dev))

        @pl.when(b == nb - 1)
        def _():
            action(remote(part.at[(2 * nb - 1) % RING, i], ready.at[nb - 1, cb + s], send_y.at[b, s], recv_y.at[b, s], y_dev))

    def add_other(slot, lower, upper):
        def one(i):
            part[slot, i] = part[slot, i] + other[i]

        loop(lower, upper, one)

    def same_send(lo):
        return jnp.logical_and(same, lax.rem(lo, 2) != x)

    def same_recv(lo):
        return jnp.logical_and(same, lax.rem(lo, 2) == x)

    def same_drain(lo):
        @pl.when(jnp.logical_not(same))
        def _():
            core_copy(lo, 0).wait_send()
            core_copy(lo, 1).wait_send()

        @pl.when(same_send(lo))
        def _():
            loop(lo, nb, lambda i: x_copy(lo, i).wait_send())

    def same_compute(lo):
        slot = lax.rem(lo, RING)

        @pl.when(lo >= RING)
        def _():
            same_drain(lo - RING)

        def one(i):
            far_copy(lo, i).wait()
            ahead = far_next(*far_next(lo, i))

            @pl.when(ahead[0] < nb)
            def _():
                far_copy(*ahead).start()

            part[slot, i] = dot_t(own[i], own[lo]) + dot_t(own[far_slot(lo, i)], own[far_slot(lo, lo)])

        loop(lo, nb, one)

        @pl.when(jnp.logical_not(same))
        def _():
            core_copy(lo, 0).start()
            core_copy(lo, 1).start()

    def same_reduce(lo):
        slot = lax.rem(lo, RING)

        @pl.when(same)
        def _():
            core_copy(lo, 0).wait_recv()
            core_copy(lo, 1).wait_recv()
            fetch(got_core.at[lo], other).wait()
            add_other(slot, lo, nb)

        @pl.when(same_send(lo))
        def _():
            loop(lo, nb, lambda i: x_copy(lo, i).start())

    def same_final(lo):
        slot = lax.rem(lo, RING)

        @pl.when(same_recv(lo))
        def _():
            loop(lo, nb, lambda i: x_copy(lo, i).wait_recv())
            fetch(got_x.at[lo], other).wait()
            above = (lax.broadcasted_iota(jnp.int32, (BLOCK, BLOCK), 0)
                     < lax.broadcasted_iota(jnp.int32, (BLOCK, BLOCK), 1))

            def one(i):
                drop = jnp.logical_or(i < lo, jnp.logical_and(i == lo, above))
                cols[pl.ds(pl.multiple_of(i * BLOCK, BLOCK), BLOCK), :] = jnp.where(
                    drop, 0.0, part[slot, i] + other[i]).astype(cols.dtype)

            loop(0, nb, one)
            s = lax.div(lo, 2)
            fetch(cols, out.at[:, pl.ds(pl.multiple_of(s * BLOCK, BLOCK), BLOCK)]).wait()

    first.wait()

    @pl.when(x == 1)
    def _():
        move.wait_recv()

    @pl.when(relays)
    def _():
        relay.start()

    loop(AHEAD, nb, start_a)

    def same_step(t):
        @pl.when(t < nb)
        def _():
            same_compute(t)

        @pl.when(jnp.logical_and(t >= 1, t <= nb))
        def _():
            same_reduce(t - 1)

        @pl.when(t >= 2)
        def _():
            same_final(t - 2)

    loop(0, nb + 2, same_step)

    def mixed_send(b, i):
        split = b + 1 - y
        stay = jnp.logical_and(jnp.logical_not(same), jnp.logical_and(i >= split, lax.rem(b, 2) != x))
        cross = jnp.logical_and(same, jnp.logical_and(i < split, lax.rem(i, 2) != x))
        return jnp.logical_or(stay, cross)

    def mixed_recv(b, i):
        split = b + 1 - y
        stay = jnp.logical_and(jnp.logical_not(same), jnp.logical_and(i >= split, lax.rem(b, 2) == x))
        cross = jnp.logical_and(same, jnp.logical_and(i < split, lax.rem(i, 2) == x))
        return jnp.logical_or(stay, cross)

    def each(cond, action, lower=0, upper=nb):
        def one(i):
            @pl.when(cond(i))
            def _():
                action(i)

        loop(lower, upper, one)

    def mixed_drain(b):
        each(lambda i: mixed_send(b, i), lambda i: x_copy(nb + b, i).wait_send())

    def mixed_reduce(b):
        job = nb + b
        slot = lax.rem(job, RING)
        split = b + 1 - y
        each(lambda i: mixed_recv(b, i), lambda i: x_copy(job, i).wait_recv())
        fetch(got_x.at[job], other).wait()

        @pl.when(jnp.logical_and(jnp.logical_not(same), lax.rem(b, 2) == x))
        def _():
            add_other(slot, split, nb)
            last = fetch(part.at[slot, nb - 1], ready.at[nb - 1, lax.div(b, 2)], 1)
            fetch(part.at[slot], kept.at[:, lax.div(b, 2)]).wait()
            last.wait()

        @pl.when(same)
        def _():
            def add(i):
                part[slot, i] = part[slot, i] + other[i]

            each(lambda i: mixed_recv(b, i), add)

            @pl.when(b < nb - 1)
            def _():
                fetch(part.at[slot], ready.at[b]).wait()

            each(lambda i: mixed_recv(b, i), lambda i: y_copy(b, i, lambda copy: copy.start()))

    @pl.when(narrow_recv)
    def _():
        own[nb, :, 0:LANES] = jnp.zeros((BLOCK, LANES), own.dtype)

    @pl.when(takes_moved)
    def _():
        relay.wait_recv()
        fetch(moved, extra.at[0]).wait()
        fetch(relayed, extra.at[1]).wait()

    def mixed_step(b):
        job = nb + b
        slot = lax.rem(job, RING)
        split = b + 1 - y

        @pl.when(b < RING)
        def _():
            same_drain(job - RING)

        @pl.when(b >= RING)
        def _():
            mixed_drain(b - RING)

        early = jnp.logical_and(b >= 1, b <= cb)

        @pl.when(b > cb)
        def _():
            mixed_reduce(b - 1)

        a_copy(b, narrow_recv, lambda copy: copy.wait_recv())

        @pl.when(narrow_recv)
        def _():
            fetch(got_a.at[b, :, pl.ds(LANES, half - LANES)], own.at[nb, :, pl.ds(LANES, half - LANES)]).wait()

        @pl.when(jnp.logical_not(narrow_recv))
        def _():
            fetch(got_a.at[b], own.at[nb]).wait()

        def one(i):
            lhs = jnp.where(i >= split, i, nb)
            rhs = jnp.where(i >= split, nb, i)
            part[slot, i] = dot_t(own[lhs], own[rhs])

        def one_extra(i):
            left = jnp.where(i >= split, 0, 1)
            part[slot, i] = part[slot, i] + dot_t(extra[left, jnp.where(i >= split, i, b)],
                                                  extra[1 - left, jnp.where(i >= split, b, i)])

        def compute_half(h):
            loop(h * cb, h * cb + cb, one)

            @pl.when(takes_moved)
            def _():
                loop(h * cb, h * cb + cb, one_extra)

            core_copy(job, h).start()

        loop(0, 2, compute_half)

        @pl.when(early)
        def _():
            mixed_reduce(b - 1)

        def reduce_half(h):
            swap = core_copy(job, h)
            swap.wait_recv()
            load = fetch(got_core.at[job, pl.ds(h * cb, cb)], other.at[pl.ds(h * cb, cb)])
            swap.wait_send()
            load.wait()
            add_other(slot, h * cb, h * cb + cb)
            each(lambda i: mixed_send(b, i), lambda i: x_copy(job, i).start(), h * cb, h * cb + cb)

        loop(0, 2, reduce_half)

    loop(0, nb, mixed_step)
    @pl.when(same)
    def _():
        mixed_reduce(jnp.int32(nb - 1))

    def finish(b):
        @pl.when(b >= nb - RING)
        def _():
            mixed_drain(b)

        a_copy(b, narrow_send, lambda copy: copy.wait_send())

    loop(0, nb, finish)

    @pl.when(x == 0)
    def _():
        move.wait_send()

    @pl.when(relays)
    def _():
        relay.wait_send()

    @pl.when(jnp.logical_not(same))
    def _():
        def wait_y(hi, s):
            @pl.when(2 * s + x < hi + y)
            def _():
                y_copy(hi, 2 * s + x, lambda copy: copy.wait_recv())

        def store_block(hi, s):
            span = pl.ds(s * BLOCK, BLOCK)
            return fetch(cols.at[span], out.at[pl.ds(pl.multiple_of(hi * BLOCK, BLOCK), BLOCK), span], s)

        def final(hi):
            mine = fetch(kept.at[hi], other.at[pl.ds(0, cb)], 0)
            loop(0, cb, lambda s: wait_y(hi, s))
            theirs = fetch(got_y.at[hi], other.at[pl.ds(cb, cb)], 1)
            mine.wait()
            theirs.wait()
            stores = []
            for s in range(cb):
                cols[s * BLOCK:(s + 1) * BLOCK, :] = jnp.where(
                    2 * s + x < hi + y, other[s] + other[cb + s], 0.0).astype(cols.dtype)
                stores.append(store_block(hi, s))
            for store in stores:
                store.wait()

        loop(0, nb - 1, final)
        mixed_reduce(jnp.int32(nb - 1))
        loop(0, cb, lambda s: wait_y(nb - 1, s))

    @pl.when(same)
    def _():
        def finish_y(b):
            each(lambda i: mixed_recv(b, i), lambda i: y_copy(b, i, lambda copy: copy.wait_send()))

        loop(0, nb, finish_y)


def store(most, sums, out, mine, theirs, cols, read_sem, bulk_sem, write_sem):
    nb = sums.shape[0]
    cb = nb // 2
    y = lax.axis_index("row")
    c = lax.axis_index("col")
    x = lax.div(c, 2)
    same = lax.rem(c, 2) == y
    head = (nb - 1) * BLOCK

    def reads(s):
        return [pltpu.make_async_copy(sums.at[nb - 1, s], mine.at[s], read_sem.at[0, s]),
                pltpu.make_async_copy(sums.at[nb - 1, cb + s], theirs.at[s], read_sem.at[1, s])]

    @pl.when(jnp.logical_not(same))
    def _():
        for s in range(cb):
            for copy in reads(s):
                copy.start()

    parts = bulk_sem.shape[0] - 1
    bulk = [pltpu.make_async_copy(most.at[pl.ds(p * head // parts, head // parts)],
                                  out.at[pl.ds(p * head // parts, head // parts)], bulk_sem.at[p])
            for p in range(parts)]
    for copy in bulk:
        copy.start()

    @pl.when(same)
    def _():
        last = pltpu.make_async_copy(most.at[pl.ds(head, BLOCK)], out.at[pl.ds(head, BLOCK)], bulk_sem.at[parts])
        last.start()
        last.wait()

    @pl.when(jnp.logical_not(same))
    def _():
        writes = []
        for s in range(cb):
            for copy in reads(s):
                copy.wait()
            cols[s] = jnp.where(2 * s + x < nb - 1 + y, mine[s] + theirs[s], 0.0).astype(cols.dtype)
            write = pltpu.make_async_copy(cols.at[s], out.at[pl.ds(head, BLOCK), pl.ds(s * BLOCK, BLOCK)],
                                          write_sem.at[s])
            write.start()
            writes.append(write)
        for write in writes:
            write.wait()

    for copy in bulk:
        copy.wait()


def solution(mesh):
    def local_fn(a_local):
        local_rows, m_local = a_local.shape
        nb = local_rows // BLOCK
        cb = nb // 2
        half = m_local // 2
        f32, bf16 = jnp.float32, a_local.dtype
        hbm = pl.BlockSpec(memory_space=pl.ANY)
        shapes = [
            jax.ShapeDtypeStruct((local_rows, cb * BLOCK), bf16),
            jax.ShapeDtypeStruct((nb, BLOCK, half), bf16),
            jax.ShapeDtypeStruct((2 * nb, nb, BLOCK, BLOCK), f32),
            jax.ShapeDtypeStruct((2 * nb, nb, BLOCK, BLOCK), f32),
            jax.ShapeDtypeStruct((nb, cb, BLOCK, BLOCK), f32),
            jax.ShapeDtypeStruct((nb, cb, BLOCK, BLOCK), f32),
            jax.ShapeDtypeStruct((nb, nb, BLOCK, BLOCK), f32),
            jax.ShapeDtypeStruct((nb, BLOCK, LANES), bf16),
            jax.ShapeDtypeStruct((nb, BLOCK, LANES), bf16),
        ]
        dma = pltpu.SemaphoreType.DMA
        outs = pl.pallas_call(
            kernel,
            out_shape=shapes,
            in_specs=[hbm],
            out_specs=[hbm] * len(shapes),
            scratch_shapes=[
                pltpu.VMEM((nb + 6, BLOCK, half), bf16),
                pltpu.VMEM((RING, nb, BLOCK, BLOCK), f32),
                pltpu.VMEM((nb, BLOCK, BLOCK), f32),
                pltpu.VMEM((local_rows, BLOCK), bf16),
                pltpu.VMEM((2, nb, BLOCK, LANES), bf16),
                dma((cb,)), dma((5,)),
                dma((nb,)), dma((nb,)),
                dma((RING, 2)), dma((2 * nb, 2)),
                dma((RING, nb)), dma((2 * nb, nb)),
                dma((nb, cb)), dma((nb, cb)),
                dma((2,)), dma((2,)),
            ],
            compiler_params=pltpu.CompilerParams(collective_id=0, has_side_effects=True,
                                                 vmem_limit_bytes=45 * 2**20),
            cost_estimate=pl.CostEstimate(flops=210 * 2 * BLOCK * BLOCK * half, bytes_accessed=400 * 2**20,
                                          transcendentals=0),
        )(a_local.reshape(nb, BLOCK, m_local))
        return pl.pallas_call(
            store,
            out_shape=shapes[0],
            in_specs=[hbm] * 2,
            out_specs=hbm,
            scratch_shapes=[
                pltpu.VMEM((cb, BLOCK, BLOCK), f32),
                pltpu.VMEM((cb, BLOCK, BLOCK), f32),
                pltpu.VMEM((cb, BLOCK, BLOCK), bf16),
                dma((2, cb)), dma((4,)), dma((cb,)),
            ],
            compiler_params=pltpu.CompilerParams(vmem_limit_bytes=45 * 2**20),
            cost_estimate=pl.CostEstimate(flops=0, bytes_accessed=2 * shapes[0].size * 2, transcendentals=0),
        )(outs[0], outs[6])

    part_spec = P(("batch", "row"), "col")
    return jax.shard_map(local_fn, mesh=mesh, in_specs=(part_spec,), out_specs=part_spec, check_vma=False)
```
